128 devices in a mesh: rows: 16 (over y, x), tp: 8 (over z, core).
Axes of the slice: x: 4, y: 4, z: 4, core: 2. Of those that a mesh axis runs over, the one named last changes fastest.
Arguments:
- train_up: bfloat16 [5120, 20480], P('rows', 'tp'), may hold values from -0.078125 to 0.078125
- low_up: bfloat16 [5120, 16], P('rows'), may hold values from -0.078125 to 0.078125
- high_up: bfloat16 [16, 20480], P(None, 'tp'), may hold values from -1.5 to 1.5
- norm_train: float32 [5120], P(('rows', 'tp')), may hold values from 0.25 to 1.75
- norm_step: float32 [5120], P(('rows', 'tp')), may hold values from -0.3 to 0.3
Outputs:
- ready_up: bfloat16 [20480, 5120], P('tp')
- serve_norm: bfloat16 [5120], replicated
The draws below stay inside these ranges and needn't reach their ends.
All inputs are finite; a program needn't handle non-finite values.
Results may differ from the reference program's by a relative error of at most 0.001.
Values may be sent and summed in bfloat16 or wider, within the bound.
A program may use at most 128 MiB of HBM per device.

```python
import jax
import jax.numpy as jnp

D_MODEL = 5120
D_INNER = 20480
RANK = 16


def shard_levels(own_key, extent, shards, smallest, high):
    def one(position, blocks):
        heights = jax.random.uniform(jax.random.fold_in(jax.random.fold_in(own_key, 6), position), (blocks,), jnp.float32, smallest / len(shards), high / len(shards))
        return jnp.repeat(jnp.exp(heights), extent[position] // blocks).reshape((-1,) + (1,) * (len(extent) - position - 1))

    level = one(*shards[0])
    for cut in shards[1:]:
        level = level * one(*cut)
    return level


def scatter_about(own_key, extent, deviation, limit, shards=(), dtype=jnp.bfloat16):
    result = jax.random.normal(own_key, extent, jnp.float32) * deviation
    if len(shards) > 0:
        result = shard_levels(own_key, extent, shards, -0.22, 0.18) * result
    return jnp.clip(result, min=-limit, max=limit).astype(dtype)


def setup_inputs(seed: int = 0) -> dict:
    keys = jax.random.split(jax.random.key(seed), 6)
    return {
        "train_up": scatter_about(keys[0], (D_MODEL, D_INNER), D_MODEL ** -0.5, 0.078125, ((0, 16), (1, 8))),
        "low_up": scatter_about(keys[1], (D_MODEL, RANK), D_MODEL ** -0.5, 0.078125, ((0, 16),)),
        "high_up": scatter_about(keys[2], (RANK, D_INNER), RANK ** -0.5, 1.5, ((1, 8),)),
        "norm_train": jnp.clip(1.0 + 0.15 * jax.random.normal(keys[3], (D_MODEL,), jnp.float32), 0.25, 1.75),
        "norm_step": jnp.clip(jax.random.uniform(keys[4], (D_MODEL,), jnp.float32, -0.3, 0.3) * shard_levels(keys[4], (D_MODEL,), ((0, 128),), -0.4, 0.0), -0.3, 0.3),
    }


mix_rate = 2.0


def reference(train_up, low_up, high_up, norm_train, norm_step):
    latest_up = train_up.astype(jnp.float32) + mix_rate * jnp.dot(low_up, high_up, preferred_element_type=jnp.float32)
    ready_up = latest_up.T.astype(jnp.bfloat16)
    serve_norm = (norm_train + norm_step).astype(jnp.bfloat16)
    return ready_up, serve_norm
```

```python
import functools

import jax
import jax.numpy as jnp
from jax import lax
from jax.experimental import pallas as pl
from jax.experimental.pallas import tpu as pltpu
from jax.sharding import PartitionSpec as P

mix_rate = 2.0
MESH = pl.DeviceIdType.MESH
SIDE = 4
LANES = 128


def ring_position(cycle, device):
    y, x = device // SIDE, device % SIDE
    return SIDE * (y if cycle == 0 else x) + (x + y) % SIDE


def ring_device(cycle, position):
    a = position // SIDE
    b = (position % SIDE + SIDE - a) % SIDE
    return SIDE * a + b if cycle == 0 else SIDE * b + a


def kernel(
    n_rows, n_tp, depth, chunks, per_ring,
    train_ref, low_ref, high_ref, normt_ref, norms_ref,
    out_ref, norm_out_ref,
    train_buf, held, norm_all,
    load_sem, send_sem, recv_sem, norm_send1, norm_recv1, norm_send2, norm_recv2,
):
    me = lax.axis_index("rows")
    my_tp = lax.axis_index("tp")
    steps = n_rows - 1

    loads = []
    for c in range(chunks):
        load = pltpu.make_async_copy(train_ref.at[:, pl.ds(c * LANES, LANES)], train_buf.at[c], load_sem.at[c])
        loads.append(load)
    order = [q * per_ring + k for k in range(per_ring) for q in range(4)]
    for c in order:
        loads[c].start()

    barrier = pltpu.get_barrier_semaphore()
    for d in range(1, n_rows):
        pl.semaphore_signal(barrier, inc=1, device_id=((me + d) % n_rows, my_tp), device_id_type=MESH)
    for d in range(1, n_tp):
        pl.semaphore_signal(barrier, inc=1, device_id=(me, (my_tp + d) % n_tp), device_id_type=MESH)
    pl.semaphore_wait(barrier, n_rows + n_tp - 2)

    def ring_copy(c, origin, to, hop):
        q = c // per_ring
        rows = pl.ds(pl.multiple_of(origin * depth, 64), depth)
        return pltpu.make_async_remote_copy(
            src_ref=held.at[c, rows, :],
            dst_ref=held.at[c, rows, :],
            send_sem=send_sem.at[c],
            recv_sem=recv_sem.at[hop, c],
            device_id=(to, my_tp),
            device_id_type=MESH,
        )

    pos = [ring_position(q // 2, me) for q in range(4)]
    way = [1 if q % 2 == 0 else n_rows - 1 for q in range(4)]
    after = [ring_device(q // 2, (pos[q] + way[q]) % n_rows) for q in range(4)]

    def turn(c, origin):
        pair, odd = origin // 2, origin % 2
        base = pl.multiple_of(pair * 2 * depth, LANES)
        top = pl.multiple_of(origin * depth, 64)
        main = held[c, pl.ds(pl.multiple_of(top + odd * 64, 64), 256), :]
        out_ref[pl.ds(c * LANES, LANES), pl.ds(pl.multiple_of(base + odd * 384, LANES), 256)] = main.T
        rest = held[c, pl.ds(pl.multiple_of(top + (1 - odd) * 256, 64), 64), :]
        rest = jnp.concatenate([rest, rest], axis=0).T
        shared = out_ref.at[pl.ds(c * LANES, LANES), pl.ds(pl.multiple_of(base + 256, LANES), LANES)]

        @pl.when(odd == 0)
        def _():
            shared[:, :64] = rest[:, :64]

        @pl.when(odd == 1)
        def _():
            shared[:, 64:] = rest[:, 64:]

    low = low_ref[...].T
    mine = pl.ds(pl.multiple_of(me * depth, 64), depth)
    before = None
    for c in order:
        delta = jnp.dot(low, high_ref[:, c * LANES:(c + 1) * LANES], preferred_element_type=jnp.float32)
        loads[c].wait()
        held[c, mine, :] = (train_buf[c].astype(jnp.float32) + mix_rate * delta).astype(jnp.bfloat16)
        if before is not None:
            ring_copy(before, me, after[before // per_ring], 0).start()
        before = c
    slot = me * n_tp + my_tp
    norm_all[slot, :, :] = jnp.zeros((1, LANES), jnp.float32)
    norm_all[slot, :, 0:normt_ref.shape[1]] = normt_ref[...] + norms_ref[...]
    ring_copy(before, me, after[before // per_ring], 0).start()

    for c in order:
        turn(c, me)

    def norm_copy1(d):
        return pltpu.make_async_remote_copy(
            src_ref=norm_all.at[slot], dst_ref=norm_all.at[slot],
            send_sem=norm_send1.at[d], recv_sem=norm_recv1.at[d],
            device_id=(me, (my_tp + d) % n_tp), device_id_type=MESH)

    def norm_copy2(d):
        group = pl.ds(me * n_tp, n_tp)
        return pltpu.make_async_remote_copy(
            src_ref=norm_all.at[group], dst_ref=norm_all.at[group],
            send_sem=norm_send2.at[d], recv_sem=norm_recv2.at[d],
            device_id=((me + d) % n_rows, my_tp), device_id_type=MESH)

    for d in range(1, n_tp):
        norm_copy1(d).start()

    def arrived(hop, forward):
        for c in order:
            q = c // per_ring
            origin = ring_device(q // 2, (pos[q] + (n_rows - way[q]) * hop) % n_rows)
            ring_copy(c, origin, after[q], hop - 1).wait_recv()
            ring_copy(c, me, after[q], 0).wait_send()
            if forward:
                ring_copy(c, origin, after[q], hop).start()
            turn(c, origin)

    arrived(1, True)
    for d in range(1, n_tp):
        norm_copy1(d).wait()
    for d in range(1, n_rows):
        norm_copy2(d).start()
    lax.fori_loop(2, steps, lambda hop, _: (arrived(hop, True), _)[1], 0)
    for d in range(1, n_rows):
        norm_copy2(d).wait()
    width = normt_ref.shape[1]
    parts = [jnp.zeros((8, LANES), jnp.float32) for _ in range(6)]
    spot = lax.broadcasted_iota(jnp.int32, (8, LANES), 1)
    for i in range(16):
        row, shift = divmod(i * width, LANES)
        x = jnp.concatenate([norm_all[16 * g + i] for g in range(8)], axis=0)
        x = pltpu.roll(x, shift, 1) if shift else x
        first = (spot >= shift) & (spot < shift + width)
        parts[row] = jnp.where(first, x, parts[row])
        if shift + width > LANES:
            parts[row + 1] = jnp.where(spot < shift + width - LANES, x, parts[row + 1])
    for g in range(8):
        for row in range(5):
            norm_out_ref[5 * g + row : 5 * g + row + 1, :] = parts[row][g : g + 1, :]
    arrived(steps, False)


def write_kernel(pieces, held_ref, norm_ref, out_ref, norm_out_ref, sems):
    rows = held_ref.shape[0] // pieces
    copies = []
    for i in range(pieces):
        part = pl.ds(i * rows, rows)
        copies.append(pltpu.make_async_copy(held_ref.at[part, :], out_ref.at[part, :], sems.at[i]))
        copies[-1].start()
    norm_out_ref[...] = norm_ref[...]
    for copy in copies:
        copy.wait()


def per_device(train_up, low_up, high_up, norm_train, norm_step):
    n_rows, n_tp = lax.axis_size("rows"), lax.axis_size("tp")
    depth, width = train_up.shape
    chunks = width // LANES
    per_ring = chunks // 4
    ready, norm = pl.pallas_call(
        functools.partial(kernel, n_rows, n_tp, depth, chunks, per_ring),
        out_shape=(
            pltpu.VMEM((width, n_rows * depth), jnp.bfloat16),
            jax.ShapeDtypeStruct((n_rows * n_tp * norm_train.shape[0] // LANES, LANES), jnp.float32),
        ),
        in_specs=[pl.BlockSpec(memory_space=pl.ANY)] + [pl.BlockSpec(memory_space=pltpu.VMEM)] * 4,
        out_specs=(pl.BlockSpec(memory_space=pltpu.VMEM), pl.BlockSpec(memory_space=pltpu.VMEM)),
        scratch_shapes=[
            pltpu.VMEM((chunks, depth, LANES), jnp.bfloat16),
            pltpu.VMEM((chunks, n_rows * depth, LANES), jnp.bfloat16),
            pltpu.VMEM((n_rows * n_tp, 1, LANES), jnp.float32),
            pltpu.SemaphoreType.DMA((chunks,)),
            pltpu.SemaphoreType.DMA((chunks,)),
            pltpu.SemaphoreType.DMA((n_rows - 1, chunks)),
            pltpu.SemaphoreType.DMA((n_tp,)),
            pltpu.SemaphoreType.DMA((n_tp,)),
            pltpu.SemaphoreType.DMA((n_rows,)),
            pltpu.SemaphoreType.DMA((n_rows,)),
        ],
        compiler_params=pltpu.CompilerParams(
            collective_id=0, has_side_effects=True, vmem_limit_bytes=30*1024*1024
        ),
    )(train_up, low_up.T, high_up, norm_train.reshape(1, -1), norm_step.reshape(1, -1))
    ready, norm = pl.pallas_call(
        functools.partial(write_kernel, 16),
        out_shape=(
            jax.ShapeDtypeStruct(ready.shape, ready.dtype),
            jax.ShapeDtypeStruct(norm.shape, norm.dtype),
        ),
        in_specs=[pl.BlockSpec(memory_space=pl.ANY), pl.BlockSpec(memory_space=pltpu.VMEM)],
        out_specs=(pl.BlockSpec(memory_space=pl.ANY), pl.BlockSpec(memory_space=pltpu.VMEM)),
        scratch_shapes=[pltpu.SemaphoreType.DMA((16,))],
        compiler_params=pltpu.CompilerParams(vmem_limit_bytes=1024 * 1024),
    )(ready, norm)
    return ready, norm.reshape(-1).astype(jnp.bfloat16)


def solution(mesh):
    placed = (P("rows", "tp"), P("rows", None), P(None, "tp"), P(("rows", "tp")), P(("rows", "tp")))
    return jax.shard_map(
        per_device, mesh=mesh, in_specs=placed, out_specs=(P("tp", None), P()), check_vma=False
    )
```

```python
import functools

import jax
import jax.numpy as jnp
from jax import lax
from jax.experimental import pallas as pl
from jax.experimental.pallas import tpu as pltpu
from jax.sharding import PartitionSpec as P

mix_rate = 2.0
MESH = pl.DeviceIdType.MESH
SIDE = 4
LANES = 128


def ring_position(cycle, device):
    y, x = device // SIDE, device % SIDE
    return SIDE * (y if cycle == 0 else x) + (x + y) % SIDE


def ring_device(cycle, position):
    a = position // SIDE
    b = (position % SIDE + SIDE - a) % SIDE
    return SIDE * a + b if cycle == 0 else SIDE * b + a


def kernel(
    n_rows, n_tp, depth, chunks, per_ring,
    train_ref, low_ref, high_ref, normt_ref, norms_ref,
    out_ref, norm_out_ref,
    train_buf, low_buf, high_buf, norm_buf, held, norm_all,
    small_sem, load_sem, send_sem, recv_sem, norm_send, norm_recv, turn_send, turn_recv,
):
    me = lax.axis_index("rows")
    my_tp = lax.axis_index("tp")
    steps = n_rows - 1
    pos = [ring_position(q // 2, me) for q in range(4)]
    way = [1 if q % 2 == 0 else n_rows - 1 for q in range(4)]
    after = [ring_device(q // 2, (pos[q] + way[q]) % n_rows) for q in range(4)]
    twin = my_tp + 1 - 2 * (my_tp % 2)
    up, down = (my_tp + 2) % n_tp, (my_tp + n_tp - 2) % n_tp

    barrier = pltpu.get_barrier_semaphore()
    for q in range(4):
        pl.semaphore_signal(barrier, inc=1, device_id=(after[q], my_tp), device_id_type=MESH)
    for other in (twin, up, down):
        pl.semaphore_signal(barrier, inc=1, device_id=(me, other), device_id_type=MESH)

    order = [q * per_ring + k for k in range(per_ring) for q in range(4)]
    small = [
        pltpu.make_async_copy(low_ref, low_buf, small_sem.at[0]),
        pltpu.make_async_copy(high_ref, high_buf, small_sem.at[1]),
        pltpu.make_async_copy(normt_ref, norm_buf.at[0], small_sem.at[2]),
        pltpu.make_async_copy(norms_ref, norm_buf.at[1], small_sem.at[3]),
    ]
    loads = [
        pltpu.make_async_copy(train_ref.at[:, pl.ds(c * LANES, LANES)], train_buf.at[c], load_sem.at[c])
        for c in range(chunks)
    ]
    for load in small:
        load.start()
    for c in order:
        loads[c].start()

    def ring_copy(c, origin, to, hop):
        rows = pl.ds(pl.multiple_of(origin * depth, 64), depth)
        return pltpu.make_async_remote_copy(
            src_ref=held.at[c, rows, :],
            dst_ref=held.at[c, rows, :],
            send_sem=send_sem.at[c],
            recv_sem=recv_sem.at[hop, c],
            device_id=(to, my_tp),
            device_id_type=MESH,
        )

    def turn(c, origin):
        pair, odd = origin // 2, origin % 2
        base = pl.multiple_of(pair * 2 * depth, LANES)
        top = pl.multiple_of(origin * depth, 64)
        main = held[c, pl.ds(pl.multiple_of(top + odd * 64, 64), 256), :]
        out_ref[pl.ds(c * LANES, LANES), pl.ds(pl.multiple_of(base + odd * 384, LANES), 256)] = main.T
        rest = held[c, pl.ds(pl.multiple_of(top + (1 - odd) * 256, 64), 64), :]
        rest = jnp.concatenate([rest, rest], axis=0).T
        shared = out_ref.at[pl.ds(c * LANES, LANES), pl.ds(pl.multiple_of(base + 256, LANES), LANES)]

        @pl.when(odd == 0)
        def _():
            shared[:, :64] = rest[:, :64]

        @pl.when(odd == 1)
        def _():
            shared[:, 64:] = rest[:, 64:]

    slot = me * n_tp + my_tp
    width = normt_ref.shape[1]

    def norm_copy(i, first, count, device):
        part = pl.ds(first, count)
        return pltpu.make_async_remote_copy(
            src_ref=norm_all.at[part], dst_ref=norm_all.at[part],
            send_sem=norm_send.at[i], recv_sem=norm_recv.at[i],
            device_id=device, device_id_type=MESH)

    def pair_of(tp):
        return me * n_tp + (tp // 2) * 2

    norm_twin = norm_copy(0, slot, 1, (me, twin))
    norm_up = norm_copy(1, pair_of(my_tp), 2, (me, up))
    norm_down = norm_copy(2, pair_of(my_tp), 2, (me, down))
    norm_far = norm_copy(3, pair_of(down), 2, (me, up))

    def norm_turn(q, hop):
        origin = ring_device(0, (pos[q] + (n_rows - way[q]) * (hop - 1)) % n_rows)
        part = pl.ds(origin * n_tp, n_tp)
        return pltpu.make_async_remote_copy(
            src_ref=norm_all.at[part], dst_ref=norm_all.at[part],
            send_sem=turn_send.at[q, hop - 1], recv_sem=turn_recv.at[q, hop - 1],
            device_id=(after[q], my_tp), device_id_type=MESH)

    reach = (n_rows // 2, (n_rows - 1) // 2)

    def norm_step(hop):
        @pl.when(hop == 1)
        def _():
            norm_twin.wait()
            norm_up.start()
            norm_down.start()

        @pl.when(hop == 2)
        def _():
            norm_up.wait()
            norm_down.wait()
            norm_far.start()

        @pl.when(hop == 3)
        def _():
            norm_far.wait()

        turn_hop = hop - 2
        for q in range(2):
            @pl.when((turn_hop > 1) & (turn_hop <= reach[q] + 1))
            def _():
                norm_turn(q, turn_hop - 1).wait()

            @pl.when((turn_hop > 0) & (turn_hop <= reach[q]))
            def _():
                norm_turn(q, turn_hop).start()

    small[0].wait()
    low = low_buf[...].T
    small[1].wait()
    pl.semaphore_wait(barrier, 7)

    mine = pl.ds(pl.multiple_of(me * depth, 64), depth)
    before = None
    for c in order:
        delta = jnp.dot(low, high_buf[:, c * LANES:(c + 1) * LANES], preferred_element_type=jnp.float32)
        loads[c].wait()
        held[c, mine, :] = (train_buf[c].astype(jnp.float32) + mix_rate * delta).astype(jnp.bfloat16)
        if before is not None:
            ring_copy(before, me, after[before // per_ring], 0).start()
        before = c
    small[2].wait()
    small[3].wait()
    norm_all[slot, :, :] = jnp.zeros((1, LANES), jnp.float32)
    norm_all[slot, :, 0:width] = norm_buf[0] + norm_buf[1]
    ring_copy(before, me, after[before // per_ring], 0).start()

    for c in order:
        turn(c, me)
    norm_twin.start()

    def arrived(hop, forward):
        for c in order:
            q = c // per_ring
            origin = ring_device(q // 2, (pos[q] + (n_rows - way[q]) * hop) % n_rows)
            ring_copy(c, origin, after[q], hop - 1).wait_recv()
            ring_copy(c, me, after[q], 0).wait_send()
            if forward:
                ring_copy(c, origin, after[q], hop).start()
            turn(c, origin)

    def body(hop, carry):
        arrived(hop, True)
        norm_step(hop)
        return carry

    lax.fori_loop(1, steps, body, 0)

    parts = [jnp.zeros((8, LANES), jnp.float32) for _ in range(6)]
    spot = lax.broadcasted_iota(jnp.int32, (8, LANES), 1)
    for i in range(16):
        row, shift = divmod(i * width, LANES)
        x = jnp.concatenate([norm_all[16 * g + i] for g in range(8)], axis=0)
        x = pltpu.roll(x, shift, 1) if shift else x
        first = (spot >= shift) & (spot < shift + width)
        parts[row] = jnp.where(first, x, parts[row])
        if shift + width > LANES:
            parts[row + 1] = jnp.where(spot < shift + width - LANES, x, parts[row + 1])
    for g in range(8):
        for row in range(5):
            norm_out_ref[5 * g + row : 5 * g + row + 1, :] = parts[row][g : g + 1, :]
    arrived(steps, False)


def write_kernel(pieces, held_ref, norm_ref, out_ref, norm_out_ref, norm_buf, sems):
    rows = held_ref.shape[0] // pieces
    copies = []
    for i in range(pieces):
        part = pl.ds(i * rows, rows)
        copies.append(pltpu.make_async_copy(held_ref.at[part, :], out_ref.at[part, :], sems.at[i]))
        copies[-1].start()
    norm_buf[...] = norm_ref[...].astype(jnp.bfloat16)
    copies.append(pltpu.make_async_copy(norm_buf, norm_out_ref, sems.at[pieces]))
    copies[-1].start()
    for copy in copies:
        copy.wait()


def per_device(train_up, low_up, high_up, norm_train, norm_step):
    n_rows, n_tp = lax.axis_size("rows"), lax.axis_size("tp")
    depth, width = train_up.shape
    rank, own = low_up.shape[1], norm_train.shape[0]
    chunks = width // LANES
    per_ring = chunks // 4
    norm_shape = (n_rows * n_tp * own // LANES, LANES)
    held, norm = pl.pallas_call(
        functools.partial(kernel, n_rows, n_tp, depth, chunks, per_ring),
        out_shape=(
            pltpu.VMEM((width, n_rows * depth), jnp.bfloat16),
            pltpu.VMEM(norm_shape, jnp.float32),
        ),
        in_specs=[pl.BlockSpec(memory_space=pl.ANY)] * 5,
        out_specs=(pl.BlockSpec(memory_space=pltpu.VMEM), pl.BlockSpec(memory_space=pltpu.VMEM)),
        scratch_shapes=[
            pltpu.VMEM((chunks, depth, LANES), jnp.bfloat16),
            pltpu.VMEM((rank, depth), jnp.bfloat16),
            pltpu.VMEM((rank, width), jnp.bfloat16),
            pltpu.VMEM((2, 1, own), jnp.float32),
            pltpu.VMEM((chunks, n_rows * depth, LANES), jnp.bfloat16),
            pltpu.VMEM((n_rows * n_tp, 1, LANES), jnp.float32),
            pltpu.SemaphoreType.DMA((4,)),
            pltpu.SemaphoreType.DMA((chunks,)),
            pltpu.SemaphoreType.DMA((chunks,)),
            pltpu.SemaphoreType.DMA((n_rows - 1, chunks)),
            pltpu.SemaphoreType.DMA((4,)),
            pltpu.SemaphoreType.DMA((4,)),
            pltpu.SemaphoreType.DMA((2, n_rows // 2)),
            pltpu.SemaphoreType.DMA((2, n_rows // 2)),
        ],
        compiler_params=pltpu.CompilerParams(
            collective_id=0, has_side_effects=True, vmem_limit_bytes=30 * 1024 * 1024
        ),
    )(train_up, low_up.T, high_up, norm_train.reshape(1, -1), norm_step.reshape(1, -1))
    pieces = 16
    ready, norm = pl.pallas_call(
        functools.partial(write_kernel, pieces),
        out_shape=(
            jax.ShapeDtypeStruct(held.shape, held.dtype),
            jax.ShapeDtypeStruct(norm_shape, jnp.bfloat16),
        ),
        in_specs=[pl.BlockSpec(memory_space=pl.ANY), pl.BlockSpec(memory_space=pltpu.VMEM)],
        out_specs=(pl.BlockSpec(memory_space=pl.ANY), pl.BlockSpec(memory_space=pl.ANY)),
        scratch_shapes=[pltpu.VMEM(norm_shape, jnp.bfloat16), pltpu.SemaphoreType.DMA((pieces + 1,))],
        compiler_params=pltpu.CompilerParams(vmem_limit_bytes=1024 * 1024),
    )(held, norm)
    return ready, norm.reshape(-1)


def solution(mesh):
    placed = (P("rows", "tp"), P("rows", None), P(None, "tp"), P(("rows", "tp")), P(("rows", "tp")))
    return jax.shard_map(
        per_device, mesh=mesh, in_specs=placed, out_specs=(P("tp", None), P()), check_vma=False
    )
```

```python
import functools

import jax
import jax.numpy as jnp
from jax import lax
from jax.experimental import pallas as pl
from jax.experimental.pallas import tpu as pltpu
from jax.sharding import PartitionSpec as P

mix_rate = 2.0
MESH = pl.DeviceIdType.MESH
SIDE = 4
LANES = 128


def ring_position(cycle, device):
    y, x = device // SIDE, device % SIDE
    return SIDE * (y if cycle == 0 else x) + (x + y) % SIDE


def ring_device(cycle, position):
    a = position // SIDE
    b = (position % SIDE + SIDE - a) % SIDE
    return SIDE * a + b if cycle == 0 else SIDE * b + a


def kernel(
    n_rows, n_tp, depth, chunks, per_ring,
    train_ref, low_ref, high_ref, normt_ref, norms_ref,
    out_ref, norm_out_ref,
    train_buf, low_buf, high_buf, norm_buf, held, norm_all,
    small_sem, load_sem, send_sem, recv_sem, norm_send, norm_recv, turn_send, turn_recv,
):
    me = lax.axis_index("rows")
    my_tp = lax.axis_index("tp")
    steps = n_rows - 1
    pos = [ring_position(q // 2, me) for q in range(4)]
    way = [1 if q % 2 == 0 else n_rows - 1 for q in range(4)]
    after = [ring_device(q // 2, (pos[q] + way[q]) % n_rows) for q in range(4)]
    twin = my_tp + 1 - 2 * (my_tp % 2)
    up, down = (my_tp + 2) % n_tp, (my_tp + n_tp - 2) % n_tp

    barrier = pltpu.get_barrier_semaphore()
    for q in range(4):
        pl.semaphore_signal(barrier, inc=1, device_id=(after[q], my_tp), device_id_type=MESH)
    for other in (twin, up, down):
        pl.semaphore_signal(barrier, inc=1, device_id=(me, other), device_id_type=MESH)

    order = [q * per_ring + k for k in range(per_ring) for q in range(4)]
    small = [
        pltpu.make_async_copy(low_ref, low_buf, small_sem.at[0]),
        pltpu.make_async_copy(high_ref, high_buf, small_sem.at[1]),
        pltpu.make_async_copy(normt_ref, norm_buf.at[0], small_sem.at[2]),
        pltpu.make_async_copy(norms_ref, norm_buf.at[1], small_sem.at[3]),
    ]
    loads = [
        pltpu.make_async_copy(train_ref.at[:, pl.ds(c * LANES, LANES)], train_buf.at[c], load_sem.at[c])
        for c in range(chunks)
    ]
    for load in small:
        load.start()
    for c in order:
        loads[c].start()

    def ring_copy(c, origin, to, hop):
        rows = pl.ds(pl.multiple_of(origin * depth, 64), depth)
        return pltpu.make_async_remote_copy(
            src_ref=held.at[c, rows, :],
            dst_ref=held.at[c, rows, :],
            send_sem=send_sem.at[c],
            recv_sem=recv_sem.at[hop, c],
            device_id=(to, my_tp),
            device_id_type=MESH,
        )

    def turn(c, origin):
        pair, odd = origin // 2, origin % 2
        base = pl.multiple_of(pair * 2 * depth, LANES)
        top = pl.multiple_of(origin * depth, 64)
        main = held[c, pl.ds(pl.multiple_of(top + odd * 64, 64), 256), :]
        out_ref[pl.ds(c * LANES, LANES), pl.ds(pl.multiple_of(base + odd * 384, LANES), 256)] = main.T
        rest = held[c, pl.ds(pl.multiple_of(top + (1 - odd) * 256, 64), 64), :]
        rest = jnp.concatenate([rest, rest], axis=0).T
        shared = out_ref.at[pl.ds(c * LANES, LANES), pl.ds(pl.multiple_of(base + 256, LANES), LANES)]

        @pl.when(odd == 0)
        def _():
            shared[:, :64] = rest[:, :64]

        @pl.when(odd == 1)
        def _():
            shared[:, 64:] = rest[:, 64:]

    slot = me * n_tp + my_tp
    width = normt_ref.shape[1]

    def norm_copy(i, first, count, device):
        part = pl.ds(first, count)
        return pltpu.make_async_remote_copy(
            src_ref=norm_all.at[part], dst_ref=norm_all.at[part],
            send_sem=norm_send.at[i], recv_sem=norm_recv.at[i],
            device_id=device, device_id_type=MESH)

    def pair_of(tp):
        return me * n_tp + (tp // 2) * 2

    norm_twin = norm_copy(0, slot, 1, (me, twin))
    norm_up = norm_copy(1, pair_of(my_tp), 2, (me, up))
    norm_down = norm_copy(2, pair_of(my_tp), 2, (me, down))
    norm_far = norm_copy(3, pair_of(down), 2, (me, up))

    def norm_turn(q, hop):
        origin = ring_device(0, (pos[q] + (n_rows - way[q]) * (hop - 1)) % n_rows)
        part = pl.ds(origin * n_tp, n_tp)
        return pltpu.make_async_remote_copy(
            src_ref=norm_all.at[part], dst_ref=norm_all.at[part],
            send_sem=turn_send.at[q, hop - 1], recv_sem=turn_recv.at[q, hop - 1],
            device_id=(after[q], my_tp), device_id_type=MESH)

    reach = (n_rows // 2, (n_rows - 1) // 2)

    def norm_step(hop):
        @pl.when(hop == 1)
        def _():
            norm_twin.wait()
            norm_up.start()
            norm_down.start()

        @pl.when(hop == 2)
        def _():
            norm_up.wait()
            norm_down.wait()
            norm_far.start()

        @pl.when(hop == 3)
        def _():
            norm_far.wait()

        turn_hop = hop - 2
        for q in range(2):
            @pl.when((turn_hop > 1) & (turn_hop <= reach[q] + 1))
            def _():
                norm_turn(q, turn_hop - 1).wait()

            @pl.when((turn_hop > 0) & (turn_hop <= reach[q]))
            def _():
                norm_turn(q, turn_hop).start()

    small[0].wait()
    low = low_buf[...].T
    small[1].wait()
    pl.semaphore_wait(barrier, 7)

    mine = pl.ds(pl.multiple_of(me * depth, 64), depth)
    before = None
    for c in order:
        delta = jnp.dot(low, high_buf[:, c * LANES:(c + 1) * LANES], preferred_element_type=jnp.float32)
        loads[c].wait()
        held[c, mine, :] = (train_buf[c].astype(jnp.float32) + mix_rate * delta).astype(jnp.bfloat16)
        if before is not None:
            ring_copy(before, me, after[before // per_ring], 0).start()
        before = c
    small[2].wait()
    small[3].wait()
    norm_all[slot, :, :] = jnp.zeros((1, LANES), jnp.float32)
    norm_all[slot, :, 0:width] = norm_buf[0] + norm_buf[1]
    ring_copy(before, me, after[before // per_ring], 0).start()

    for c in order:
        turn(c, me)
    norm_twin.start()

    def arrived(hop, forward):
        for c in order:
            q = c // per_ring
            origin = ring_device(q // 2, (pos[q] + (n_rows - way[q]) * hop) % n_rows)
            ring_copy(c, origin, after[q], hop - 1).wait_recv()
            ring_copy(c, me, after[q], 0).wait_send()
            if forward:
                ring_copy(c, origin, after[q], hop).start()
            turn(c, origin)

    def body(hop, carry):
        arrived(hop, True)
        norm_step(hop)
        return carry

    lax.fori_loop(1, steps, body, 0)

    parts = [jnp.zeros((8, LANES), jnp.float32) for _ in range(6)]
    spot = lax.broadcasted_iota(jnp.int32, (8, LANES), 1)
    for i in range(16):
        row, shift = divmod(i * width, LANES)
        x = jnp.concatenate([norm_all[16 * g + i] for g in range(8)], axis=0)
        x = pltpu.roll(x, shift, 1) if shift else x
        first = (spot >= shift) & (spot < shift + width)
        parts[row] = jnp.where(first, x, parts[row])
        if shift + width > LANES:
            parts[row + 1] = jnp.where(spot < shift + width - LANES, x, parts[row + 1])
    for g in range(8):
        for row in range(5):
            norm_out_ref[5 * g + row : 5 * g + row + 1, :] = parts[row][g : g + 1, :]
    arrived(steps, False)


def scoped_kernel(n_rows, n_tp, depth, chunks, per_ring, *refs):
    sem = pltpu.SemaphoreType.DMA
    pl.run_scoped(
        functools.partial(kernel, n_rows, n_tp, depth, chunks, per_ring, *refs),
        sem((4,)), sem((chunks,)), sem((chunks,)), sem((n_rows - 1, chunks)),
        sem((4,)), sem((4,)), sem((2, n_rows // 2)), sem((2, n_rows // 2)),
    )


def write_kernel(pieces, held_ref, norm_ref, out_ref, norm_out_ref, norm_buf, sems):
    rows = held_ref.shape[0] // pieces
    copies = []
    for i in range(pieces):
        part = pl.ds(i * rows, rows)
        copies.append(pltpu.make_async_copy(held_ref.at[part, :], out_ref.at[part, :], sems.at[i]))
        copies[-1].start()
    norm_buf[...] = norm_ref[...].astype(jnp.bfloat16)
    copies.append(pltpu.make_async_copy(norm_buf, norm_out_ref, sems.at[pieces]))
    copies[-1].start()
    for copy in copies:
        copy.wait()


def per_device(train_up, low_up, high_up, norm_train, norm_step):
    n_rows, n_tp = lax.axis_size("rows"), lax.axis_size("tp")
    depth, width = train_up.shape
    rank, own = low_up.shape[1], norm_train.shape[0]
    chunks = width // LANES
    per_ring = chunks // 4
    norm_shape = (n_rows * n_tp * own // LANES, LANES)
    held, norm = pl.pallas_call(
        functools.partial(scoped_kernel, n_rows, n_tp, depth, chunks, per_ring),
        out_shape=(
            pltpu.VMEM((width, n_rows * depth), jnp.bfloat16),
            pltpu.VMEM(norm_shape, jnp.float32),
        ),
        in_specs=[pl.BlockSpec(memory_space=pl.ANY)] * 5,
        out_specs=(pl.BlockSpec(memory_space=pltpu.VMEM), pl.BlockSpec(memory_space=pltpu.VMEM)),
        scratch_shapes=[
            pltpu.VMEM((chunks, depth, LANES), jnp.bfloat16),
            pltpu.VMEM((rank, depth), jnp.bfloat16),
            pltpu.VMEM((rank, width), jnp.bfloat16),
            pltpu.VMEM((2, 1, own), jnp.float32),
            pltpu.VMEM((chunks, n_rows * depth, LANES), jnp.bfloat16),
            pltpu.VMEM((n_rows * n_tp, 1, LANES), jnp.float32),
        ],
        compiler_params=pltpu.CompilerParams(
            collective_id=0, has_side_effects=True, vmem_limit_bytes=30 * 1024 * 1024
        ),
    )(train_up, low_up.T, high_up, norm_train.reshape(1, -1), norm_step.reshape(1, -1))
    pieces = 16
    ready, norm = pl.pallas_call(
        functools.partial(write_kernel, pieces),
        out_shape=(
            jax.ShapeDtypeStruct(held.shape, held.dtype),
            jax.ShapeDtypeStruct(norm_shape, jnp.bfloat16),
        ),
        in_specs=[pl.BlockSpec(memory_space=pl.ANY), pl.BlockSpec(memory_space=pltpu.VMEM)],
        out_specs=(pl.BlockSpec(memory_space=pl.ANY), pl.BlockSpec(memory_space=pl.ANY)),
        scratch_shapes=[pltpu.VMEM(norm_shape, jnp.bfloat16), pltpu.SemaphoreType.DMA((pieces + 1,))],
        compiler_params=pltpu.CompilerParams(vmem_limit_bytes=1024 * 1024),
    )(held, norm)
    return ready, norm.reshape(-1)


def solution(mesh):
    placed = (P("rows", "tp"), P("rows", None), P(None, "tp"), P(("rows", "tp")), P(("rows", "tp")))
    return jax.shard_map(
        per_device, mesh=mesh, in_specs=placed, out_specs=(P("tp", None), P()), check_vma=False
    )
```

```python
import functools

import jax
import jax.numpy as jnp
from jax import lax
from jax.experimental import pallas as pl
from jax.experimental.pallas import tpu as pltpu
from jax.sharding import PartitionSpec as P

mix_rate = 2.0
MESH = pl.DeviceIdType.MESH
SPLIT = 3
SIDE = 4
LANES = 128


def ring_position(cycle, device):
    y, x = device // SIDE, device % SIDE
    return SIDE * (y if cycle == 0 else x) + (x + y) % SIDE


def ring_device(cycle, position):
    a = position // SIDE
    b = (position % SIDE + SIDE - a) % SIDE
    return SIDE * a + b if cycle == 0 else SIDE * b + a


def put_half(tile, value, half):
    @pl.when(half == 0)
    def _():
        tile[:, :64] = value[:, :64]

    @pl.when(half == 1)
    def _():
        tile[:, 64:] = value[:, 64:]


def splits(tp):
    return 1 - tp % 2


def kernel(
    n_rows, n_tp, depth, chunks, per_ring,
    train_ref, low_ref, high_ref, normt_ref, norms_ref,
    out_ref, mine_ref, norm_out_ref,
    train_buf, low_buf, high_buf, norm_buf, held, norm_all,
    small_sem, load_sem, send_sem, recv_sem, norm_send, norm_recv, turn_send, turn_recv,
):
    me = lax.axis_index("rows")
    my_tp = lax.axis_index("tp")
    steps = n_rows - 1 - SPLIT * splits(my_tp)
    pos = [ring_position(q // 2, me) for q in range(4)]
    way = [1 if q % 2 == 0 else n_rows - 1 for q in range(4)]
    after = [ring_device(q // 2, (pos[q] + way[q]) % n_rows) for q in range(4)]
    twin = my_tp + 1 - 2 * (my_tp % 2)
    up, down = (my_tp + 2) % n_tp, (my_tp + n_tp - 2) % n_tp

    barrier = pltpu.get_barrier_semaphore()
    for q in range(4):
        pl.semaphore_signal(barrier, inc=1, device_id=(after[q], my_tp), device_id_type=MESH)
    for other in (twin, up, down):
        pl.semaphore_signal(barrier, inc=1, device_id=(me, other), device_id_type=MESH)

    order = [q * per_ring + k for k in range(per_ring) for q in range(4)]
    small = [
        pltpu.make_async_copy(low_ref, low_buf, small_sem.at[0]),
        pltpu.make_async_copy(high_ref, high_buf, small_sem.at[1]),
        pltpu.make_async_copy(normt_ref, norm_buf.at[0], small_sem.at[2]),
        pltpu.make_async_copy(norms_ref, norm_buf.at[1], small_sem.at[3]),
    ]
    loads = [
        pltpu.make_async_copy(train_ref.at[:, pl.ds(c * LANES, LANES)], train_buf.at[c], load_sem.at[c])
        for c in range(chunks)
    ]
    for load in small:
        load.start()
    for c in order:
        loads[c].start()

    def ring_copy(c, origin, to, hop, first=False):
        rows = pl.ds(pl.multiple_of(origin * depth, 64), depth)
        return pltpu.make_async_remote_copy(
            src_ref=mine_ref.at[c] if first else held.at[c, rows, :],
            dst_ref=held.at[c, rows, :],
            send_sem=send_sem.at[c],
            recv_sem=recv_sem.at[hop, c],
            device_id=(to, my_tp),
            device_id_type=MESH,
        )

    def turn(c, origin, first=False):
        pair, odd = origin // 2, origin % 2
        base = pl.multiple_of(pair * 2 * depth, LANES)
        top = 0 if first else origin * depth
        source = mine_ref if first else held
        main = source[c, pl.ds(pl.multiple_of(top + odd * 64, 64), 256), :]
        out_ref[pl.ds(c * LANES, LANES), pl.ds(pl.multiple_of(base + odd * 384, LANES), 256)] = main.T
        rest = source[c, pl.ds(pl.multiple_of(top + (1 - odd) * 256, 64), 64), :]
        rest = jnp.concatenate([rest, rest], axis=0).T
        shared = out_ref.at[pl.ds(c * LANES, LANES), pl.ds(pl.multiple_of(base + 256, LANES), LANES)]
        put_half(shared, rest, odd)

    slot = me * n_tp + my_tp
    width = normt_ref.shape[1]

    def norm_copy(i, first, count, device):
        part = pl.ds(first, count)
        return pltpu.make_async_remote_copy(
            src_ref=norm_all.at[part], dst_ref=norm_all.at[part],
            send_sem=norm_send.at[i], recv_sem=norm_recv.at[i],
            device_id=device, device_id_type=MESH)

    def pair_of(tp):
        return me * n_tp + (tp // 2) * 2

    norm_twin = norm_copy(0, slot, 1, (me, twin))
    norm_up = norm_copy(1, pair_of(my_tp), 2, (me, up))
    norm_down = norm_copy(2, pair_of(my_tp), 2, (me, down))
    norm_far = norm_copy(3, pair_of(down), 2, (me, up))

    def norm_turn(q, hop):
        origin = ring_device(0, (pos[q] + (n_rows - way[q]) * (hop - 1)) % n_rows)
        part = pl.ds(origin * n_tp, n_tp)
        return pltpu.make_async_remote_copy(
            src_ref=norm_all.at[part], dst_ref=norm_all.at[part],
            send_sem=turn_send.at[q, hop - 1], recv_sem=turn_recv.at[q, hop - 1],
            device_id=(after[q], my_tp), device_id_type=MESH)

    reach = (n_rows // 2, (n_rows - 1) // 2)

    def norm_step(hop):
        @pl.when(hop == 1)
        def _():
            norm_twin.wait()
            norm_up.start()
            norm_down.start()

        @pl.when(hop == 2)
        def _():
            norm_up.wait()
            norm_down.wait()
            norm_far.start()

        @pl.when(hop == 3)
        def _():
            norm_far.wait()

        turn_hop = hop - 2
        for q in range(2):
            @pl.when((turn_hop > 1) & (turn_hop <= reach[q] + 1))
            def _():
                norm_turn(q, turn_hop - 1).wait()

            @pl.when((turn_hop > 0) & (turn_hop <= reach[q]))
            def _():
                norm_turn(q, turn_hop).start()

    small[0].wait()
    low = low_buf[...].T
    small[1].wait()
    pl.semaphore_wait(barrier, 7)

    before = None
    for c in order:
        delta = jnp.dot(low, high_buf[:, c * LANES:(c + 1) * LANES], preferred_element_type=jnp.float32)
        loads[c].wait()
        mine_ref[c] = (train_buf[c].astype(jnp.float32) + mix_rate * delta).astype(jnp.bfloat16)
        if before is not None:
            ring_copy(before, me, after[before // per_ring], 0, True).start()
        before = c
    small[2].wait()
    small[3].wait()
    norm_all[slot, :, :] = jnp.zeros((1, LANES), jnp.float32)
    norm_all[slot, :, 0:width] = norm_buf[0] + norm_buf[1]
    ring_copy(before, me, after[before // per_ring], 0, True).start()

    for c in order:
        turn(c, me, True)
    norm_twin.start()

    def arrived(hop, forward):
        for c in order:
            q = c // per_ring
            origin = ring_device(q // 2, (pos[q] + (n_rows - way[q]) * hop) % n_rows)
            ring_copy(c, origin, after[q], hop - 1).wait_recv()
            ring_copy(c, me, after[q], 0, True).wait_send()
            if forward:
                ring_copy(c, origin, after[q], hop).start()
            turn(c, origin)

    def body(hop, carry):
        arrived(hop, True)
        norm_step(hop)
        return carry

    lax.fori_loop(1, steps, body, 0)

    parts = [jnp.zeros((8, LANES), jnp.float32) for _ in range(6)]
    spot = lax.broadcasted_iota(jnp.int32, (8, LANES), 1)
    for i in range(16):
        row, shift = divmod(i * width, LANES)
        x = jnp.concatenate([norm_all[16 * g + i] for g in range(8)], axis=0)
        x = pltpu.roll(x, shift, 1) if shift else x
        first = (spot >= shift) & (spot < shift + width)
        parts[row] = jnp.where(first, x, parts[row])
        if shift + width > LANES:
            parts[row + 1] = jnp.where(spot < shift + width - LANES, x, parts[row + 1])
    for g in range(8):
        for row in range(5):
            norm_out_ref[5 * g + row : 5 * g + row + 1, :] = parts[row][g : g + 1, :]
    arrived(steps, False)


def scoped_kernel(n_rows, n_tp, depth, chunks, per_ring, *refs):
    sem = pltpu.SemaphoreType.DMA
    pl.run_scoped(
        functools.partial(kernel, n_rows, n_tp, depth, chunks, per_ring, *refs),
        sem((4,)), sem((chunks,)), sem((chunks,)), sem((n_rows - 1, chunks)),
        sem((4,)), sem((4,)), sem((2, n_rows // 2)), sem((2, n_rows // 2)),
    )


def late_place(n_rows, q, me, away):
    position, way = ring_position(q // 2, me), 1 if q % 2 == 0 else n_rows - 1
    origin = ring_device(q // 2, (position + way * away) % n_rows)
    other = origin + 1 - 2 * (origin % 2)
    gap = (ring_position(q // 2, other) + n_rows - position) * way % n_rows
    return origin, gap


def late_kernel(
    n_rows, depth, chunks, per_ring, first_ref, mine_ref, patch_ref, late, stash, send_sem, recv_sem, stash_sem
):
    me = lax.axis_index("rows")
    my_tp = lax.axis_index("tp")
    order = [q * per_ring + k for k in range(per_ring) for q in range(4)]

    def neighbour(q, step):
        way = 1 if q % 2 == 0 else n_rows - 1
        return ring_device(q // 2, (ring_position(q // 2, me) + step * way) % n_rows)

    def late_copy(c, hop, first):
        q = c // per_ring
        return pltpu.make_async_remote_copy(
            src_ref=mine_ref.at[c] if first else late.at[hop - 1, c],
            dst_ref=late.at[hop, c],
            send_sem=send_sem.at[c],
            recv_sem=recv_sem.at[hop, c],
            device_id=(neighbour(q, n_rows - 1), my_tp),
            device_id_type=MESH,
        )

    def stash_copy(q, slot):
        origin, _ = late_place(n_rows, q, me, slot + 1)
        rows = pl.ds(q * per_ring * LANES, per_ring * LANES)
        lanes = pl.ds(pl.multiple_of(origin // 2 * 2 * depth + 256, LANES), LANES)
        return pltpu.make_async_copy(first_ref.at[rows, lanes], stash.at[slot, rows, :], stash_sem.at[slot, q])

    def turn(c, slot):
        q = c // per_ring
        origin, gap = late_place(n_rows, q, me, slot + 1)
        odd = origin % 2
        rows = pl.ds(c * LANES, LANES)
        main = late[slot, c, pl.ds(pl.multiple_of(odd * 64, 64), 256), :]
        patch_ref[slot, rows, 0:256] = main.T
        rest = late[slot, c, pl.ds(pl.multiple_of((1 - odd) * 256, 64), 64), :]
        shared = patch_ref.at[slot, rows, 256:384]
        put_half(shared, jnp.concatenate([rest, rest], axis=0).T, odd)

        @pl.when((gap == 0) | (gap > SPLIT))
        def _():
            put_half(shared, stash[slot, rows, :], 1 - odd)

        @pl.when((gap > 0) & (gap <= slot))
        def _():
            put_half(shared, patch_ref[gap - 1, rows, 256:384], 1 - odd)

    @pl.when(splits(my_tp) == 1)
    def _():
        barrier = pltpu.get_barrier_semaphore()
        for q in range(4):
            pl.semaphore_signal(barrier, inc=1, device_id=(neighbour(q, 1), my_tp), device_id_type=MESH)
        pl.semaphore_wait(barrier, 4)
        for c in order:
            late_copy(c, 0, True).start()
        stashed = [stash_copy(q, slot) for slot in range(SPLIT) for q in range(4)]
        for copy in stashed:
            copy.start()
        for copy in stashed:
            copy.wait()
        for hop in range(SPLIT):
            for c in order:
                late_copy(c, hop, hop == 0).wait()
                if hop + 1 < SPLIT:
                    late_copy(c, hop + 1, False).start()
                turn(c, hop)


def scoped_late_kernel(n_rows, depth, chunks, per_ring, *refs):
    sem = pltpu.SemaphoreType.DMA
    pl.run_scoped(
        functools.partial(late_kernel, n_rows, depth, chunks, per_ring, *refs),
        sem((chunks,)), sem((SPLIT, chunks)), sem((SPLIT, 4)),
    )


def write_kernel(pieces, held_ref, norm_ref, out_ref, norm_out_ref, norm_buf, sems):
    rows = held_ref.shape[0] // pieces
    copies = []
    for i in range(pieces):
        part = pl.ds(i * rows, rows)
        copies.append(pltpu.make_async_copy(held_ref.at[part, :], out_ref.at[part, :], sems.at[i]))
        copies[-1].start()
    norm_buf[...] = norm_ref[...].astype(jnp.bfloat16)
    copies.append(pltpu.make_async_copy(norm_buf, norm_out_ref, sems.at[pieces]))
    copies[-1].start()
    for copy in copies:
        copy.wait()


def patch_kernel(n_rows, depth, quarter, patch_ref, first_ref, out_ref, main_sem, shared_sem):
    me = lax.axis_index("rows")

    def copies(q, slot):
        origin, gap = late_place(n_rows, q, me, slot + 1)
        base = origin // 2 * 2 * depth
        rows = pl.ds(q * quarter, quarter)
        lanes = pl.ds(pl.multiple_of(base + origin % 2 * 384, LANES), 256)
        shared_lanes = pl.ds(pl.multiple_of(base + 256, LANES), LANES)
        main = pltpu.make_async_copy(patch_ref.at[slot, rows, 0:256], out_ref.at[rows, lanes], main_sem.at[slot, q])
        shared = pltpu.make_async_copy(
            patch_ref.at[slot, rows, 256:384], out_ref.at[rows, shared_lanes], shared_sem.at[slot, q])
        return main, shared, (gap <= slot) | (gap > SPLIT)

    @pl.when(splits(lax.axis_index("tp")) == 1)
    def _():
        everything = [copies(q, slot) for slot in range(SPLIT) for q in range(4)]
        for main, shared, last in everything:
            main.start()
            pl.when(last)(shared.start)
        for main, shared, last in everything:
            main.wait()
            pl.when(last)(shared.wait)


def per_device(train_up, low_up, high_up, norm_train, norm_step):
    n_rows, n_tp = lax.axis_size("rows"), lax.axis_size("tp")
    depth, width = train_up.shape
    rank, own = low_up.shape[1], norm_train.shape[0]
    chunks = width // LANES
    per_ring = chunks // 4
    norm_shape = (n_rows * n_tp * own // LANES, LANES)
    anywhere, vmem = pl.BlockSpec(memory_space=pl.ANY), pl.BlockSpec(memory_space=pltpu.VMEM)
    held, mine, norm = pl.pallas_call(
        functools.partial(scoped_kernel, n_rows, n_tp, depth, chunks, per_ring),
        out_shape=(
            pltpu.VMEM((width, n_rows * depth), jnp.bfloat16),
            pltpu.VMEM((chunks, depth, LANES), jnp.bfloat16),
            pltpu.VMEM(norm_shape, jnp.float32),
        ),
        in_specs=[anywhere] * 5,
        out_specs=(vmem, vmem, vmem),
        scratch_shapes=[
            pltpu.VMEM((chunks, depth, LANES), jnp.bfloat16),
            pltpu.VMEM((rank, depth), jnp.bfloat16),
            pltpu.VMEM((rank, width), jnp.bfloat16),
            pltpu.VMEM((2, 1, own), jnp.float32),
            pltpu.VMEM((chunks, n_rows * depth, LANES), jnp.bfloat16),
            pltpu.VMEM((n_rows * n_tp, 1, LANES), jnp.float32),
        ],
        compiler_params=pltpu.CompilerParams(
            collective_id=0, has_side_effects=True, vmem_limit_bytes=30 * 1024 * 1024
        ),
    )(train_up, low_up.T, high_up, norm_train.reshape(1, -1), norm_step.reshape(1, -1))
    pieces = 16
    first, norm = pl.pallas_call(
        functools.partial(write_kernel, pieces),
        out_shape=(
            jax.ShapeDtypeStruct(held.shape, held.dtype),
            jax.ShapeDtypeStruct(norm_shape, jnp.bfloat16),
        ),
        in_specs=[anywhere, vmem],
        out_specs=(anywhere, anywhere),
        scratch_shapes=[pltpu.VMEM(norm_shape, jnp.bfloat16), pltpu.SemaphoreType.DMA((pieces + 1,))],
        compiler_params=pltpu.CompilerParams(vmem_limit_bytes=1024 * 1024),
    )(held, norm)
    patch = pl.pallas_call(
        functools.partial(scoped_late_kernel, n_rows, depth, chunks, per_ring),
        out_shape=pltpu.VMEM((SPLIT, width, 384), jnp.bfloat16),
        in_specs=[anywhere, vmem],
        out_specs=vmem,
        scratch_shapes=[
            pltpu.VMEM((SPLIT, chunks, depth, LANES), jnp.bfloat16),
            pltpu.VMEM((SPLIT, width, LANES), jnp.bfloat16),
        ],
        compiler_params=pltpu.CompilerParams(
            collective_id=1, has_side_effects=True, vmem_limit_bytes=40 * 1024 * 1024
        ),
    )(first, mine)
    ready = pl.pallas_call(
        functools.partial(patch_kernel, n_rows, depth, width // 4),
        out_shape=jax.ShapeDtypeStruct(held.shape, held.dtype),
        in_specs=[anywhere, anywhere],
        out_specs=anywhere,
        input_output_aliases={1: 0},
        scratch_shapes=[pltpu.SemaphoreType.DMA((SPLIT, 4)), pltpu.SemaphoreType.DMA((SPLIT, 4))],
        compiler_params=pltpu.CompilerParams(vmem_limit_bytes=1024 * 1024),
    )(patch, first)
    return ready, norm.reshape(-1)


def solution(mesh):
    placed = (P("rows", "tp"), P("rows", None), P(None, "tp"), P(("rows", "tp")), P(("rows", "tp")))
    return jax.shard_map(
        per_device, mesh=mesh, in_specs=placed, out_specs=(P("tp", None), P()), check_vma=False
    )
```

```python
import functools

import jax
import jax.numpy as jnp
from jax import lax
from jax.experimental import pallas as pl
from jax.experimental.pallas import tpu as pltpu
from jax.sharding import PartitionSpec as P

mix_rate = 2.0
MESH = pl.DeviceIdType.MESH
SPLIT = 3
SIDE = 4
LANES = 128


def ring_position(cycle, device):
    y, x = device // SIDE, device % SIDE
    return SIDE * (y if cycle == 0 else x) + (x + y) % SIDE


def ring_device(cycle, position):
    a = position // SIDE
    b = (position % SIDE + SIDE - a) % SIDE
    return SIDE * a + b if cycle == 0 else SIDE * b + a


def put_half(tile, value, half):
    @pl.when(half == 0)
    def _():
        tile[:, :64] = value[:, :64]

    @pl.when(half == 1)
    def _():
        tile[:, 64:] = value[:, 64:]


def splits(tp):
    return tp % 2


def kernel(
    n_rows, n_tp, depth, chunks, per_ring,
    train_ref, low_ref, high_ref, normt_ref, norms_ref,
    out_ref, mine_ref, norm_out_ref,
    train_buf, low_buf, high_buf, norm_buf, held, norm_all,
    small_sem, load_sem, send_sem, recv_sem, norm_send, norm_recv, turn_send, turn_recv,
):
    me = lax.axis_index("rows")
    my_tp = lax.axis_index("tp")
    steps = n_rows - 1 - SPLIT * splits(my_tp)
    pos = [ring_position(q // 2, me) for q in range(4)]
    way = [1 if q % 2 == 0 else n_rows - 1 for q in range(4)]
    after = [ring_device(q // 2, (pos[q] + way[q]) % n_rows) for q in range(4)]
    twin = my_tp + 1 - 2 * (my_tp % 2)
    up, down = (my_tp + 2) % n_tp, (my_tp + n_tp - 2) % n_tp

    barrier = pltpu.get_barrier_semaphore()
    for q in range(4):
        pl.semaphore_signal(barrier, inc=1, device_id=(after[q], my_tp), device_id_type=MESH)
    for other in (twin, up, down):
        pl.semaphore_signal(barrier, inc=1, device_id=(me, other), device_id_type=MESH)

    order = [q * per_ring + k for k in range(per_ring) for q in range(4)]
    small = [
        pltpu.make_async_copy(low_ref, low_buf, small_sem.at[0]),
        pltpu.make_async_copy(high_ref, high_buf, small_sem.at[1]),
        pltpu.make_async_copy(normt_ref, norm_buf.at[0], small_sem.at[2]),
        pltpu.make_async_copy(norms_ref, norm_buf.at[1], small_sem.at[3]),
    ]
    loads = [
        pltpu.make_async_copy(train_ref.at[:, pl.ds(c * LANES, LANES)], train_buf.at[c], load_sem.at[c])
        for c in range(chunks)
    ]
    for load in small:
        load.start()
    for c in order:
        loads[c].start()

    def ring_copy(c, origin, to, hop, first=False):
        rows = pl.ds(pl.multiple_of(origin * depth, 64), depth)
        return pltpu.make_async_remote_copy(
            src_ref=mine_ref.at[c] if first else held.at[c, rows, :],
            dst_ref=held.at[c, rows, :],
            send_sem=send_sem.at[c],
            recv_sem=recv_sem.at[hop, c],
            device_id=(to, my_tp),
            device_id_type=MESH,
        )

    def turn(c, origin, first=False):
        pair, odd = origin // 2, origin % 2
        base = pl.multiple_of(pair * 2 * depth, LANES)
        top = 0 if first else origin * depth
        source = mine_ref if first else held
        main = source[c, pl.ds(pl.multiple_of(top + odd * 64, 64), 256), :]
        out_ref[pl.ds(c * LANES, LANES), pl.ds(pl.multiple_of(base + odd * 384, LANES), 256)] = main.T
        rest = source[c, pl.ds(pl.multiple_of(top + (1 - odd) * 256, 64), 64), :]
        rest = jnp.concatenate([rest, rest], axis=0).T
        shared = out_ref.at[pl.ds(c * LANES, LANES), pl.ds(pl.multiple_of(base + 256, LANES), LANES)]
        put_half(shared, rest, odd)

    slot = me * n_tp + my_tp
    width = normt_ref.shape[1]

    def norm_copy(i, first, count, device):
        part = pl.ds(first, count)
        return pltpu.make_async_remote_copy(
            src_ref=norm_all.at[part], dst_ref=norm_all.at[part],
            send_sem=norm_send.at[i], recv_sem=norm_recv.at[i],
            device_id=device, device_id_type=MESH)

    def pair_of(tp):
        return me * n_tp + (tp // 2) * 2

    norm_twin = norm_copy(0, slot, 1, (me, twin))
    norm_up = norm_copy(1, pair_of(my_tp), 2, (me, up))
    norm_down = norm_copy(2, pair_of(my_tp), 2, (me, down))
    norm_far = norm_copy(3, pair_of(down), 2, (me, up))

    def norm_turn(q, hop):
        origin = ring_device(0, (pos[q] + (n_rows - way[q]) * (hop - 1)) % n_rows)
        part = pl.ds(origin * n_tp, n_tp)
        return pltpu.make_async_remote_copy(
            src_ref=norm_all.at[part], dst_ref=norm_all.at[part],
            send_sem=turn_send.at[q, hop - 1], recv_sem=turn_recv.at[q, hop - 1],
            device_id=(after[q], my_tp), device_id_type=MESH)

    reach = (n_rows // 2, (n_rows - 1) // 2)

    def norm_step(hop):
        @pl.when(hop == 1)
        def _():
            norm_twin.wait()
            norm_up.start()
            norm_down.start()

        @pl.when(hop == 2)
        def _():
            norm_up.wait()
            norm_down.wait()
            norm_far.start()

        @pl.when(hop == 3)
        def _():
            norm_far.wait()

        turn_hop = hop - 2
        for q in range(2):
            @pl.when((turn_hop > 1) & (turn_hop <= reach[q] + 1))
            def _():
                norm_turn(q, turn_hop - 1).wait()

            @pl.when((turn_hop > 0) & (turn_hop <= reach[q]))
            def _():
                norm_turn(q, turn_hop).start()

    small[0].wait()
    low = low_buf[...].T
    small[1].wait()
    before = None
    for c in order:
        delta = jnp.dot(low, high_buf[:, c * LANES:(c + 1) * LANES], preferred_element_type=jnp.float32)
        loads[c].wait()
        mine_ref[c] = (train_buf[c].astype(jnp.float32) + mix_rate * delta).astype(jnp.bfloat16)
        if c == order[1]:
            pl.semaphore_wait(barrier, 7)
        if before is not None:
            ring_copy(before, me, after[before // per_ring], 0, True).start()
        before = c
    small[2].wait()
    small[3].wait()
    norm_all[slot, :, :] = jnp.zeros((1, LANES), jnp.float32)
    norm_all[slot, :, 0:width] = norm_buf[0] + norm_buf[1]
    ring_copy(before, me, after[before // per_ring], 0, True).start()

    for c in order:
        turn(c, me, True)
    norm_twin.start()

    def arrived(hop, forward):
        for c in order:
            q = c // per_ring
            origin = ring_device(q // 2, (pos[q] + (n_rows - way[q]) * hop) % n_rows)
            ring_copy(c, origin, after[q], hop - 1).wait_recv()
            ring_copy(c, me, after[q], 0, True).wait_send()
            if forward:
                ring_copy(c, origin, after[q], hop).start()
            turn(c, origin)

    def body(hop, carry):
        arrived(hop, True)
        norm_step(hop)
        return carry

    lax.fori_loop(1, steps, body, 0)

    parts = [jnp.zeros((8, LANES), jnp.float32) for _ in range(6)]
    spot = lax.broadcasted_iota(jnp.int32, (8, LANES), 1)
    for i in range(16):
        row, shift = divmod(i * width, LANES)
        x = jnp.concatenate([norm_all[16 * g + i] for g in range(8)], axis=0)
        x = pltpu.roll(x, shift, 1) if shift else x
        first = (spot >= shift) & (spot < shift + width)
        parts[row] = jnp.where(first, x, parts[row])
        if shift + width > LANES:
            parts[row + 1] = jnp.where(spot < shift + width - LANES, x, parts[row + 1])
    for g in range(8):
        for row in range(5):
            norm_out_ref[5 * g + row : 5 * g + row + 1, :] = parts[row][g : g + 1, :]
    arrived(steps, False)


def scoped_kernel(n_rows, n_tp, depth, chunks, per_ring, *refs):
    sem = pltpu.SemaphoreType.DMA
    pl.run_scoped(
        functools.partial(kernel, n_rows, n_tp, depth, chunks, per_ring, *refs),
        sem((4,)), sem((chunks,)), sem((chunks,)), sem((n_rows - 1, chunks)),
        sem((4,)), sem((4,)), sem((2, n_rows // 2)), sem((2, n_rows // 2)),
    )


def late_place(n_rows, q, me, away):
    position, way = ring_position(q // 2, me), 1 if q % 2 == 0 else n_rows - 1
    origin = ring_device(q // 2, (position + way * away) % n_rows)
    other = origin + 1 - 2 * (origin % 2)
    gap = (ring_position(q // 2, other) + n_rows - position) * way % n_rows
    return origin, gap


def late_kernel(
    n_rows, depth, chunks, per_ring, first_ref, mine_ref, patch_ref, late, stash, send_sem, recv_sem, stash_sem
):
    me = lax.axis_index("rows")
    my_tp = lax.axis_index("tp")
    order = [q * per_ring + k for k in range(per_ring) for q in range(4)]

    def neighbour(q, step):
        way = 1 if q % 2 == 0 else n_rows - 1
        return ring_device(q // 2, (ring_position(q // 2, me) + step * way) % n_rows)

    def late_copy(c, hop, first):
        q = c // per_ring
        return pltpu.make_async_remote_copy(
            src_ref=mine_ref.at[c] if first else late.at[hop - 1, c],
            dst_ref=late.at[hop, c],
            send_sem=send_sem.at[c],
            recv_sem=recv_sem.at[hop, c],
            device_id=(neighbour(q, n_rows - 1), my_tp),
            device_id_type=MESH,
        )

    def stash_copy(q, slot):
        origin, _ = late_place(n_rows, q, me, slot + 1)
        rows = pl.ds(q * per_ring * LANES, per_ring * LANES)
        lanes = pl.ds(pl.multiple_of(origin // 2 * 2 * depth + 256, LANES), LANES)
        return pltpu.make_async_copy(first_ref.at[rows, lanes], stash.at[slot, rows, :], stash_sem.at[slot, q])

    def turn(c, slot):
        q = c // per_ring
        origin, gap = late_place(n_rows, q, me, slot + 1)
        odd = origin % 2
        rows = pl.ds(c * LANES, LANES)
        main = late[slot, c, pl.ds(pl.multiple_of(odd * 64, 64), 256), :]
        patch_ref[slot, rows, 0:256] = main.T
        rest = late[slot, c, pl.ds(pl.multiple_of((1 - odd) * 256, 64), 64), :]
        shared = patch_ref.at[slot, rows, 256:384]
        put_half(shared, jnp.concatenate([rest, rest], axis=0).T, odd)

        @pl.when((gap == 0) | (gap > SPLIT))
        def _():
            put_half(shared, stash[slot, rows, :], 1 - odd)

        @pl.when((gap > 0) & (gap <= slot))
        def _():
            put_half(shared, patch_ref[gap - 1, rows, 256:384], 1 - odd)

    @pl.when(splits(my_tp) == 1)
    def _():
        barrier = pltpu.get_barrier_semaphore()
        for q in range(4):
            pl.semaphore_signal(barrier, inc=1, device_id=(neighbour(q, 1), my_tp), device_id_type=MESH)
        pl.semaphore_wait(barrier, 4)
        for c in order:
            late_copy(c, 0, True).start()
        stashed = [stash_copy(q, slot) for slot in range(SPLIT) for q in range(4)]
        for copy in stashed:
            copy.start()
        for copy in stashed:
            copy.wait()
        for hop in range(SPLIT):
            for c in order:
                late_copy(c, hop, hop == 0).wait()
                if hop + 1 < SPLIT:
                    late_copy(c, hop + 1, False).start()
                turn(c, hop)


def scoped_late_kernel(n_rows, depth, chunks, per_ring, *refs):
    sem = pltpu.SemaphoreType.DMA
    pl.run_scoped(
        functools.partial(late_kernel, n_rows, depth, chunks, per_ring, *refs),
        sem((chunks,)), sem((SPLIT, chunks)), sem((SPLIT, 4)),
    )


def write_kernel(pieces, held_ref, norm_ref, out_ref, norm_out_ref, norm_buf, sems):
    rows = held_ref.shape[0] // pieces
    copies = []
    for i in range(pieces):
        part = pl.ds(i * rows, rows)
        copies.append(pltpu.make_async_copy(held_ref.at[part, :], out_ref.at[part, :], sems.at[i]))
        copies[-1].start()
    norm_buf[...] = norm_ref[...].astype(jnp.bfloat16)
    copies.append(pltpu.make_async_copy(norm_buf, norm_out_ref, sems.at[pieces]))
    copies[-1].start()
    for copy in copies:
        copy.wait()


def patch_kernel(n_rows, depth, quarter, patch_ref, first_ref, out_ref, main_sem, shared_sem):
    me = lax.axis_index("rows")

    def copies(q, slot):
        origin, gap = late_place(n_rows, q, me, slot + 1)
        base = origin // 2 * 2 * depth
        rows = pl.ds(q * quarter, quarter)
        lanes = pl.ds(pl.multiple_of(base + origin % 2 * 384, LANES), 256)
        shared_lanes = pl.ds(pl.multiple_of(base + 256, LANES), LANES)
        main = pltpu.make_async_copy(patch_ref.at[slot, rows, 0:256], out_ref.at[rows, lanes], main_sem.at[slot, q])
        shared = pltpu.make_async_copy(
            patch_ref.at[slot, rows, 256:384], out_ref.at[rows, shared_lanes], shared_sem.at[slot, q])
        return main, shared, (gap <= slot) | (gap > SPLIT)

    @pl.when(splits(lax.axis_index("tp")) == 1)
    def _():
        everything = [copies(q, slot) for slot in range(SPLIT) for q in range(4)]
        for main, shared, last in everything:
            main.start()
            pl.when(last)(shared.start)
        for main, shared, last in everything:
            main.wait()
            pl.when(last)(shared.wait)


def per_device(train_up, low_up, high_up, norm_train, norm_step):
    n_rows, n_tp = lax.axis_size("rows"), lax.axis_size("tp")
    depth, width = train_up.shape
    rank, own = low_up.shape[1], norm_train.shape[0]
    chunks = width // LANES
    per_ring = chunks // 4
    norm_shape = (n_rows * n_tp * own // LANES, LANES)
    anywhere, vmem = pl.BlockSpec(memory_space=pl.ANY), pl.BlockSpec(memory_space=pltpu.VMEM)
    held, mine, norm = pl.pallas_call(
        functools.partial(scoped_kernel, n_rows, n_tp, depth, chunks, per_ring),
        out_shape=(
            pltpu.VMEM((width, n_rows * depth), jnp.bfloat16),
            pltpu.VMEM((chunks, depth, LANES), jnp.bfloat16),
            pltpu.VMEM(norm_shape, jnp.float32),
        ),
        in_specs=[anywhere] * 5,
        out_specs=(vmem, vmem, vmem),
        scratch_shapes=[
            pltpu.VMEM((chunks, depth, LANES), jnp.bfloat16),
            pltpu.VMEM((rank, depth), jnp.bfloat16),
            pltpu.VMEM((rank, width), jnp.bfloat16),
            pltpu.VMEM((2, 1, own), jnp.float32),
            pltpu.VMEM((chunks, n_rows * depth, LANES), jnp.bfloat16),
            pltpu.VMEM((n_rows * n_tp, 1, LANES), jnp.float32),
        ],
        compiler_params=pltpu.CompilerParams(
            collective_id=0, has_side_effects=True, vmem_limit_bytes=30 * 1024 * 1024
        ),
    )(train_up, low_up.T, high_up, norm_train.reshape(1, -1), norm_step.reshape(1, -1))
    pieces = 16
    first, norm = pl.pallas_call(
        functools.partial(write_kernel, pieces),
        out_shape=(
            jax.ShapeDtypeStruct(held.shape, held.dtype),
            jax.ShapeDtypeStruct(norm_shape, jnp.bfloat16),
        ),
        in_specs=[anywhere, vmem],
        out_specs=(anywhere, anywhere),
        scratch_shapes=[pltpu.VMEM(norm_shape, jnp.bfloat16), pltpu.SemaphoreType.DMA((pieces + 1,))],
        compiler_params=pltpu.CompilerParams(vmem_limit_bytes=1024 * 1024),
    )(held, norm)
    patch = pl.pallas_call(
        functools.partial(scoped_late_kernel, n_rows, depth, chunks, per_ring),
        out_shape=pltpu.VMEM((SPLIT, width, 384), jnp.bfloat16),
        in_specs=[anywhere, vmem],
        out_specs=vmem,
        scratch_shapes=[
            pltpu.VMEM((SPLIT, chunks, depth, LANES), jnp.bfloat16),
            pltpu.VMEM((SPLIT, width, LANES), jnp.bfloat16),
        ],
        compiler_params=pltpu.CompilerParams(
            collective_id=1, has_side_effects=True, vmem_limit_bytes=40 * 1024 * 1024
        ),
    )(first, mine)
    ready = pl.pallas_call(
        functools.partial(patch_kernel, n_rows, depth, width // 4),
        out_shape=jax.ShapeDtypeStruct(held.shape, held.dtype),
        in_specs=[anywhere, anywhere],
        out_specs=anywhere,
        input_output_aliases={1: 0},
        scratch_shapes=[pltpu.SemaphoreType.DMA((SPLIT, 4)), pltpu.SemaphoreType.DMA((SPLIT, 4))],
        compiler_params=pltpu.CompilerParams(vmem_limit_bytes=1024 * 1024),
    )(patch, first)
    return ready, norm.reshape(-1)


def solution(mesh):
    placed = (P("rows", "tp"), P("rows", None), P(None, "tp"), P(("rows", "tp")), P(("rows", "tp")))
    return jax.shard_map(
        per_device, mesh=mesh, in_specs=placed, out_specs=(P("tp", None), P()), check_vma=False
    )
```

```python
import functools

import jax
import jax.numpy as jnp
from jax import lax
from jax.experimental import pallas as pl
from jax.experimental.pallas import tpu as pltpu
from jax.sharding import PartitionSpec as P

mix_rate = 2.0
MESH = pl.DeviceIdType.MESH
SPLIT = 3
SIDE = 4
LANES = 128


def ring_position(cycle, device):
    y, x = device // SIDE, device % SIDE
    return SIDE * (y if cycle == 0 else x) + (x + y) % SIDE


def ring_device(cycle, position):
    a = position // SIDE
    b = (position % SIDE + SIDE - a) % SIDE
    return SIDE * a + b if cycle == 0 else SIDE * b + a


def put_half(tile, value, half):
    @pl.when(half == 0)
    def _():
        tile[:, :64] = value[:, :64]

    @pl.when(half == 1)
    def _():
        tile[:, 64:] = value[:, 64:]


def splits(tp):
    return tp % 2


def kernel(
    n_rows, n_tp, depth, chunks, per_ring,
    train_ref, low_ref, high_ref, normt_ref, norms_ref,
    out_ref, mine_ref, norm_out_ref,
    train_buf, low_buf, high_buf, norm_buf, held, norm_all, norm_lines, norm_line,
    small_sem, load_sem, send_sem, recv_sem, norm_send, norm_recv, turn_send, turn_recv, line_send, line_recv,
):
    me = lax.axis_index("rows")
    my_tp = lax.axis_index("tp")
    steps = n_rows - 1 - SPLIT * splits(my_tp)
    pos = [ring_position(q // 2, me) for q in range(4)]
    way = [1 if q % 2 == 0 else n_rows - 1 for q in range(4)]
    after = [ring_device(q // 2, (pos[q] + way[q]) % n_rows) for q in range(4)]
    twin = my_tp + 1 - 2 * (my_tp % 2)
    up, down = (my_tp + 2) % n_tp, (my_tp + n_tp - 2) % n_tp

    barrier = pltpu.get_barrier_semaphore()
    for q in range(4):
        pl.semaphore_signal(barrier, inc=1, device_id=(after[q], my_tp), device_id_type=MESH)
    gateway = me == 0

    @pl.when(gateway)
    def _():
        for other in (twin, up, down):
            pl.semaphore_signal(barrier, inc=1, device_id=(me, other), device_id_type=MESH)

    order = [q * per_ring + k for k in range(per_ring) for q in range(4)]
    small = [
        pltpu.make_async_copy(low_ref, low_buf, small_sem.at[0]),
        pltpu.make_async_copy(high_ref, high_buf, small_sem.at[1]),
        pltpu.make_async_copy(normt_ref, norm_buf.at[0], small_sem.at[2]),
        pltpu.make_async_copy(norms_ref, norm_buf.at[1], small_sem.at[3]),
    ]
    loads = [
        pltpu.make_async_copy(train_ref.at[:, pl.ds(c * LANES, LANES)], train_buf.at[c], load_sem.at[c])
        for c in range(chunks)
    ]
    for load in small:
        load.start()
    for c in order:
        loads[c].start()

    def ring_copy(c, origin, to, hop, first=False):
        rows = pl.ds(pl.multiple_of(origin * depth, 64), depth)
        return pltpu.make_async_remote_copy(
            src_ref=mine_ref.at[c] if first else held.at[c, rows, :],
            dst_ref=held.at[c, rows, :],
            send_sem=send_sem.at[c],
            recv_sem=recv_sem.at[hop, c],
            device_id=(to, my_tp),
            device_id_type=MESH,
        )

    def turn(c, origin, first=False):
        pair, odd = origin // 2, origin % 2
        base = pl.multiple_of(pair * 2 * depth, LANES)
        top = 0 if first else origin * depth
        source = mine_ref if first else held
        main = source[c, pl.ds(pl.multiple_of(top + odd * 64, 64), 256), :]
        out_ref[pl.ds(c * LANES, LANES), pl.ds(pl.multiple_of(base + odd * 384, LANES), 256)] = main.T
        rest = source[c, pl.ds(pl.multiple_of(top + (1 - odd) * 256, 64), 64), :]
        rest = jnp.concatenate([rest, rest], axis=0).T
        shared = out_ref.at[pl.ds(c * LANES, LANES), pl.ds(pl.multiple_of(base + 256, LANES), LANES)]
        put_half(shared, rest, odd)

    slot = my_tp * n_rows + me
    width = normt_ref.shape[1]

    def norm_copy(i, first, count, other):
        part = pl.ds(first * n_rows, count * n_rows)
        return pltpu.make_async_remote_copy(
            src_ref=norm_all.at[part], dst_ref=norm_all.at[part],
            send_sem=norm_send.at[i], recv_sem=norm_recv.at[i],
            device_id=(me, other), device_id_type=MESH)

    norm_twin = norm_copy(0, my_tp, 1, twin)
    norm_up = norm_copy(1, my_tp // 2 * 2, 2, up)
    norm_down = norm_copy(2, my_tp // 2 * 2, 2, down)
    norm_far = norm_copy(3, down // 2 * 2, 2, up)

    def norm_turn(q, hop):
        origin = ring_device(0, (pos[q] + (n_rows - way[q]) * (hop - 1)) % n_rows)
        part = pl.ds(my_tp * n_rows + origin, 1)
        return pltpu.make_async_remote_copy(
            src_ref=norm_all.at[part], dst_ref=norm_all.at[part],
            send_sem=turn_send.at[q, hop - 1], recv_sem=turn_recv.at[q, hop - 1],
            device_id=(after[q], my_tp), device_id_type=MESH)

    def norm_pass(q):
        return pltpu.make_async_remote_copy(
            src_ref=norm_line, dst_ref=norm_line, send_sem=line_send.at[q], recv_sem=line_recv.at[q],
            device_id=(after[q], my_tp), device_id_type=MESH)

    reach = (n_rows // 2, (n_rows - 1) // 2)
    far = (pos[0], (n_rows - pos[0]) % n_rows)
    passes = [far[q] < reach[q] for q in range(2)]
    takes = [(far[q] > 0) & (far[q] <= reach[q]) for q in range(2)]
    meet = n_rows // 2

    def assemble():
        parts = [jnp.zeros((8, LANES), jnp.float32) for _ in range(6)]
        spot = lax.broadcasted_iota(jnp.int32, (8, LANES), 1)
        for i in range(16):
            row, shift = divmod(i * width, LANES)
            x = jnp.concatenate([norm_all[i % 8 * n_rows + 2 * g + i // 8] for g in range(8)], axis=0)
            x = pltpu.roll(x, shift, 1) if shift else x
            first = (spot >= shift) & (spot < shift + width)
            parts[row] = jnp.where(first, x, parts[row])
            if shift + width > LANES:
                parts[row + 1] = jnp.where(spot < shift + width - LANES, x, parts[row + 1])
        for g in range(8):
            for row in range(5):
                norm_lines[5 * g + row : 5 * g + row + 1, :] = parts[row][g : g + 1, :]
        norm_line[...] = norm_lines[...].astype(jnp.bfloat16)

    def norm_step(half):
        for q in range(2):
            @pl.when((half > 0) & (half <= reach[q]))
            def _():
                norm_turn(q, half).wait()

            @pl.when(half < reach[q])
            def _():
                norm_turn(q, half + 1).start()

        @pl.when(gateway & (half == meet))
        def _():
            norm_twin.start()

        @pl.when(gateway & (half == meet + 1))
        def _():
            norm_twin.wait()
            norm_up.start()
            norm_down.start()

        @pl.when(gateway & (half == meet + 2))
        def _():
            norm_up.wait()
            norm_down.wait()
            norm_far.start()

        @pl.when(gateway & (half == meet + 3))
        def _():
            norm_far.wait()
            assemble()

        for q in range(2):
            @pl.when(half == meet + 4 + far[q])
            def _():
                pl.when(takes[q])(lambda: norm_pass(q).wait_recv())
                pl.when(passes[q])(lambda: norm_pass(q).start())

    small[0].wait()
    low = low_buf[...].T
    small[1].wait()
    before = None
    for c in order:
        delta = jnp.dot(low, high_buf[:, c * LANES:(c + 1) * LANES], preferred_element_type=jnp.float32)
        loads[c].wait()
        mine_ref[c] = (train_buf[c].astype(jnp.float32) + mix_rate * delta).astype(jnp.bfloat16)
        if c == order[1]:
            pl.semaphore_wait(barrier, jnp.where(gateway, 7, 4))
        if before is not None:
            ring_copy(before, me, after[before // per_ring], 0, True).start()
        before = c
    small[2].wait()
    small[3].wait()
    norm_all[slot, :, :] = jnp.zeros((1, LANES), jnp.float32)
    norm_all[slot, :, 0:width] = norm_buf[0] + norm_buf[1]
    ring_copy(before, me, after[before // per_ring], 0, True).start()

    for c in order:
        turn(c, me, True)

    def arrived(hop, forward):
        for i, c in enumerate(order):
            q = c // per_ring
            origin = ring_device(q // 2, (pos[q] + (n_rows - way[q]) * hop) % n_rows)
            ring_copy(c, origin, after[q], hop - 1).wait_recv()
            ring_copy(c, me, after[q], 0, True).wait_send()
            if forward:
                ring_copy(c, origin, after[q], hop).start()
            turn(c, origin)
            if forward and (i + 1) % (chunks // 2) == 0:
                norm_step(2 * (hop - 1) + (i + 1) // (chunks // 2) - 1)

    def body(hop, carry):
        arrived(hop, True)
        return carry

    lax.fori_loop(1, steps, body, 0)

    for q in range(2):
        pl.when(passes[q])(lambda: norm_pass(q).wait_send())
    norm_out_ref[...] = norm_line[...]
    arrived(steps, False)


def scoped_kernel(n_rows, n_tp, depth, chunks, per_ring, *refs):
    sem = pltpu.SemaphoreType.DMA
    pl.run_scoped(
        functools.partial(kernel, n_rows, n_tp, depth, chunks, per_ring, *refs),
        sem((4,)), sem((chunks,)), sem((chunks,)), sem((n_rows - 1, chunks)),
        sem((4,)), sem((4,)), sem((2, n_rows // 2)), sem((2, n_rows // 2)), sem((2,)), sem((2,)),
    )


def late_place(n_rows, q, me, away):
    position, way = ring_position(q // 2, me), 1 if q % 2 == 0 else n_rows - 1
    origin = ring_device(q // 2, (position + way * away) % n_rows)
    other = origin + 1 - 2 * (origin % 2)
    gap = (ring_position(q // 2, other) + n_rows - position) * way % n_rows
    return origin, gap


def late_kernel(
    n_rows, depth, chunks, per_ring, first_ref, mine_ref, patch_ref, late, stash, send_sem, recv_sem, stash_sem
):
    me = lax.axis_index("rows")
    my_tp = lax.axis_index("tp")
    order = [q * per_ring + k for k in range(per_ring) for q in range(4)]

    def neighbour(q, step):
        way = 1 if q % 2 == 0 else n_rows - 1
        return ring_device(q // 2, (ring_position(q // 2, me) + step * way) % n_rows)

    def late_copy(c, hop, first):
        q = c // per_ring
        return pltpu.make_async_remote_copy(
            src_ref=mine_ref.at[c] if first else late.at[hop - 1, c],
            dst_ref=late.at[hop, c],
            send_sem=send_sem.at[c],
            recv_sem=recv_sem.at[hop, c],
            device_id=(neighbour(q, n_rows - 1), my_tp),
            device_id_type=MESH,
        )

    def stash_copy(q, slot):
        origin, _ = late_place(n_rows, q, me, slot + 1)
        rows = pl.ds(q * per_ring * LANES, per_ring * LANES)
        lanes = pl.ds(pl.multiple_of(origin // 2 * 2 * depth + 256, LANES), LANES)
        return pltpu.make_async_copy(first_ref.at[rows, lanes], stash.at[slot, rows, :], stash_sem.at[slot, q])

    def turn(c, slot):
        q = c // per_ring
        origin, gap = late_place(n_rows, q, me, slot + 1)
        odd = origin % 2
        rows = pl.ds(c * LANES, LANES)
        main = late[slot, c, pl.ds(pl.multiple_of(odd * 64, 64), 256), :]
        patch_ref[slot, rows, 0:256] = main.T
        rest = late[slot, c, pl.ds(pl.multiple_of((1 - odd) * 256, 64), 64), :]
        shared = patch_ref.at[slot, rows, 256:384]
        put_half(shared, jnp.concatenate([rest, rest], axis=0).T, odd)

        @pl.when((gap == 0) | (gap > SPLIT))
        def _():
            put_half(shared, stash[slot, rows, :], 1 - odd)

        @pl.when((gap > 0) & (gap <= slot))
        def _():
            put_half(shared, patch_ref[gap - 1, rows, 256:384], 1 - odd)

    @pl.when(splits(my_tp) == 1)
    def _():
        barrier = pltpu.get_barrier_semaphore()
        for q in range(4):
            pl.semaphore_signal(barrier, inc=1, device_id=(neighbour(q, 1), my_tp), device_id_type=MESH)
        pl.semaphore_wait(barrier, 4)
        for c in order:
            late_copy(c, 0, True).start()
        stashed = [stash_copy(q, slot) for slot in range(SPLIT) for q in range(4)]
        for copy in stashed:
            copy.start()
        for copy in stashed:
            copy.wait()
        for hop in range(SPLIT):
            for c in order:
                late_copy(c, hop, hop == 0).wait()
                if hop + 1 < SPLIT:
                    late_copy(c, hop + 1, False).start()
                turn(c, hop)


def scoped_late_kernel(n_rows, depth, chunks, per_ring, *refs):
    sem = pltpu.SemaphoreType.DMA
    pl.run_scoped(
        functools.partial(late_kernel, n_rows, depth, chunks, per_ring, *refs),
        sem((chunks,)), sem((SPLIT, chunks)), sem((SPLIT, 4)),
    )


def write_kernel(pieces, held_ref, norm_ref, out_ref, norm_out_ref, sems):
    rows = held_ref.shape[0] // pieces
    copies = []
    for i in range(pieces):
        part = pl.ds(i * rows, rows)
        copies.append(pltpu.make_async_copy(held_ref.at[part, :], out_ref.at[part, :], sems.at[i]))
        copies[-1].start()
    copies.append(pltpu.make_async_copy(norm_ref, norm_out_ref, sems.at[pieces]))
    copies[-1].start()
    for copy in copies:
        copy.wait()


def patch_kernel(n_rows, depth, quarter, patch_ref, first_ref, out_ref, main_sem, shared_sem):
    me = lax.axis_index("rows")

    def copies(q, slot):
        origin, gap = late_place(n_rows, q, me, slot + 1)
        base = origin // 2 * 2 * depth
        rows = pl.ds(q * quarter, quarter)
        lanes = pl.ds(pl.multiple_of(base + origin % 2 * 384, LANES), 256)
        shared_lanes = pl.ds(pl.multiple_of(base + 256, LANES), LANES)
        main = pltpu.make_async_copy(patch_ref.at[slot, rows, 0:256], out_ref.at[rows, lanes], main_sem.at[slot, q])
        shared = pltpu.make_async_copy(
            patch_ref.at[slot, rows, 256:384], out_ref.at[rows, shared_lanes], shared_sem.at[slot, q])
        return main, shared, (gap <= slot) | (gap > SPLIT)

    @pl.when(splits(lax.axis_index("tp")) == 1)
    def _():
        everything = [copies(q, slot) for slot in range(SPLIT) for q in range(4)]
        for main, shared, last in everything:
            main.start()
            pl.when(last)(shared.start)
        for main, shared, last in everything:
            main.wait()
            pl.when(last)(shared.wait)


def per_device(train_up, low_up, high_up, norm_train, norm_step):
    n_rows, n_tp = lax.axis_size("rows"), lax.axis_size("tp")
    depth, width = train_up.shape
    rank, own = low_up.shape[1], norm_train.shape[0]
    chunks = width // LANES
    per_ring = chunks // 4
    norm_shape = (n_rows * n_tp * own // LANES, LANES)
    anywhere, vmem = pl.BlockSpec(memory_space=pl.ANY), pl.BlockSpec(memory_space=pltpu.VMEM)
    held, mine, norm = pl.pallas_call(
        functools.partial(scoped_kernel, n_rows, n_tp, depth, chunks, per_ring),
        out_shape=(
            pltpu.VMEM((width, n_rows * depth), jnp.bfloat16),
            pltpu.VMEM((chunks, depth, LANES), jnp.bfloat16),
            pltpu.VMEM(norm_shape, jnp.bfloat16),
        ),
        in_specs=[anywhere] * 5,
        out_specs=(vmem, vmem, vmem),
        scratch_shapes=[
            pltpu.VMEM((chunks, depth, LANES), jnp.bfloat16),
            pltpu.VMEM((rank, depth), jnp.bfloat16),
            pltpu.VMEM((rank, width), jnp.bfloat16),
            pltpu.VMEM((2, 1, own), jnp.float32),
            pltpu.VMEM((chunks, n_rows * depth, LANES), jnp.bfloat16),
            pltpu.VMEM((n_rows * n_tp, 1, LANES), jnp.float32),
            pltpu.VMEM(norm_shape, jnp.float32),
            pltpu.VMEM(norm_shape, jnp.bfloat16),
        ],
        compiler_params=pltpu.CompilerParams(
            collective_id=0, has_side_effects=True, vmem_limit_bytes=30 * 1024 * 1024
        ),
    )(train_up, low_up.T, high_up, norm_train.reshape(1, -1), norm_step.reshape(1, -1))
    pieces = 16
    first, norm = pl.pallas_call(
        functools.partial(write_kernel, pieces),
        out_shape=(
            jax.ShapeDtypeStruct(held.shape, held.dtype),
            jax.ShapeDtypeStruct(norm_shape, jnp.bfloat16),
        ),
        in_specs=[anywhere, anywhere],
        out_specs=(anywhere, anywhere),
        scratch_shapes=[pltpu.SemaphoreType.DMA((pieces + 1,))],
        compiler_params=pltpu.CompilerParams(vmem_limit_bytes=1024 * 1024),
    )(held, norm)
    patch = pl.pallas_call(
        functools.partial(scoped_late_kernel, n_rows, depth, chunks, per_ring),
        out_shape=pltpu.VMEM((SPLIT, width, 384), jnp.bfloat16),
        in_specs=[anywhere, vmem],
        out_specs=vmem,
        scratch_shapes=[
            pltpu.VMEM((SPLIT, chunks, depth, LANES), jnp.bfloat16),
            pltpu.VMEM((SPLIT, width, LANES), jnp.bfloat16),
        ],
        compiler_params=pltpu.CompilerParams(
            collective_id=1, has_side_effects=True, vmem_limit_bytes=40 * 1024 * 1024
        ),
    )(first, mine)
    ready = pl.pallas_call(
        functools.partial(patch_kernel, n_rows, depth, width // 4),
        out_shape=jax.ShapeDtypeStruct(held.shape, held.dtype),
        in_specs=[anywhere, anywhere],
        out_specs=anywhere,
        input_output_aliases={1: 0},
        scratch_shapes=[pltpu.SemaphoreType.DMA((SPLIT, 4)), pltpu.SemaphoreType.DMA((SPLIT, 4))],
        compiler_params=pltpu.CompilerParams(vmem_limit_bytes=1024 * 1024),
    )(patch, first)
    return ready, norm.reshape(-1)


def solution(mesh):
    placed = (P("rows", "tp"), P("rows", None), P(None, "tp"), P(("rows", "tp")), P(("rows", "tp")))
    return jax.shard_map(
        per_device, mesh=mesh, in_specs=placed, out_specs=(P("tp", None), P()), check_vma=False
    )
```

```python
import functools

import jax
import jax.numpy as jnp
from jax import lax
from jax.experimental import pallas as pl
from jax.experimental.pallas import tpu as pltpu
from jax.sharding import PartitionSpec as P

mix_rate = 2.0
MESH = pl.DeviceIdType.MESH
SPLIT = 4
SIDE = 4
LANES = 128


def ring_position(cycle, device):
    y, x = device // SIDE, device % SIDE
    return SIDE * (y if cycle == 0 else x) + (x + y) % SIDE


def ring_device(cycle, position):
    a = position // SIDE
    b = (position % SIDE + SIDE - a) % SIDE
    return SIDE * a + b if cycle == 0 else SIDE * b + a


def put_half(tile, value, half):
    @pl.when(half == 0)
    def _():
        tile[:, :64] = value[:, :64]

    @pl.when(half == 1)
    def _():
        tile[:, 64:] = value[:, 64:]


def splits(tp):
    return 1 + (SPLIT - 1) * (tp % 2)


def kernel(
    n_rows, n_tp, depth, chunks, per_ring,
    train_ref, low_ref, high_ref, normt_ref, norms_ref,
    out_ref, mine_ref, norm_out_ref,
    train_buf, low_buf, high_buf, norm_buf, held, norm_all, norm_lines, norm_line,
    small_sem, load_sem, send_sem, recv_sem, norm_send, norm_recv, turn_send, turn_recv, line_send, line_recv,
):
    me = lax.axis_index("rows")
    my_tp = lax.axis_index("tp")
    steps = n_rows - 1 - splits(my_tp)
    pos = [ring_position(q // 2, me) for q in range(4)]
    way = [1 if q % 2 == 0 else n_rows - 1 for q in range(4)]
    after = [ring_device(q // 2, (pos[q] + way[q]) % n_rows) for q in range(4)]
    twin = my_tp + 1 - 2 * (my_tp % 2)
    up, down = (my_tp + 2) % n_tp, (my_tp + n_tp - 2) % n_tp

    barrier = pltpu.get_barrier_semaphore()
    for q in range(4):
        pl.semaphore_signal(barrier, inc=1, device_id=(after[q], my_tp), device_id_type=MESH)
    gateway = me == 0

    @pl.when(gateway)
    def _():
        for other in (twin, up, down):
            pl.semaphore_signal(barrier, inc=1, device_id=(me, other), device_id_type=MESH)

    order = [q * per_ring + k for k in range(per_ring) for q in range(4)]
    small = [
        pltpu.make_async_copy(low_ref, low_buf, small_sem.at[0]),
        pltpu.make_async_copy(high_ref, high_buf, small_sem.at[1]),
        pltpu.make_async_copy(normt_ref, norm_buf.at[0], small_sem.at[2]),
        pltpu.make_async_copy(norms_ref, norm_buf.at[1], small_sem.at[3]),
    ]
    loads = [
        pltpu.make_async_copy(train_ref.at[:, pl.ds(c * LANES, LANES)], train_buf.at[c], load_sem.at[c])
        for c in range(chunks)
    ]
    for load in small:
        load.start()
    for c in order:
        loads[c].start()

    def ring_copy(c, origin, to, hop, first=False):
        rows = pl.ds(pl.multiple_of(origin * depth, 64), depth)
        return pltpu.make_async_remote_copy(
            src_ref=mine_ref.at[c] if first else held.at[c, rows, :],
            dst_ref=held.at[c, rows, :],
            send_sem=send_sem.at[c],
            recv_sem=recv_sem.at[hop, c],
            device_id=(to, my_tp),
            device_id_type=MESH,
        )

    def turn(c, origin, first=False):
        pair, odd = origin // 2, origin % 2
        base = pl.multiple_of(pair * 2 * depth, LANES)
        top = 0 if first else origin * depth
        source = mine_ref if first else held
        main = source[c, pl.ds(pl.multiple_of(top + odd * 64, 64), 256), :]
        out_ref[pl.ds(c * LANES, LANES), pl.ds(pl.multiple_of(base + odd * 384, LANES), 256)] = main.T
        rest = source[c, pl.ds(pl.multiple_of(top + (1 - odd) * 256, 64), 64), :]
        rest = jnp.concatenate([rest, rest], axis=0).T
        shared = out_ref.at[pl.ds(c * LANES, LANES), pl.ds(pl.multiple_of(base + 256, LANES), LANES)]
        put_half(shared, rest, odd)

    slot = my_tp * n_rows + me
    width = normt_ref.shape[1]

    def norm_copy(i, first, count, other):
        part = pl.ds(first * n_rows, count * n_rows)
        return pltpu.make_async_remote_copy(
            src_ref=norm_all.at[part], dst_ref=norm_all.at[part],
            send_sem=norm_send.at[i], recv_sem=norm_recv.at[i],
            device_id=(me, other), device_id_type=MESH)

    norm_twin = norm_copy(0, my_tp, 1, twin)
    norm_up = norm_copy(1, my_tp // 2 * 2, 2, up)
    norm_down = norm_copy(2, my_tp // 2 * 2, 2, down)
    norm_far = norm_copy(3, down // 2 * 2, 2, up)

    def norm_turn(q, hop):
        origin = ring_device(0, (pos[q] + (n_rows - way[q]) * (hop - 1)) % n_rows)
        part = pl.ds(my_tp * n_rows + origin, 1)
        return pltpu.make_async_remote_copy(
            src_ref=norm_all.at[part], dst_ref=norm_all.at[part],
            send_sem=turn_send.at[q, hop - 1], recv_sem=turn_recv.at[q, hop - 1],
            device_id=(after[q], my_tp), device_id_type=MESH)

    def norm_pass(q):
        return pltpu.make_async_remote_copy(
            src_ref=norm_line, dst_ref=norm_line, send_sem=line_send.at[q], recv_sem=line_recv.at[q],
            device_id=(after[q], my_tp), device_id_type=MESH)

    reach = (n_rows // 2, (n_rows - 1) // 2)
    far = (pos[0], (n_rows - pos[0]) % n_rows)
    passes = [far[q] < reach[q] for q in range(2)]
    takes = [(far[q] > 0) & (far[q] <= reach[q]) for q in range(2)]
    meet = n_rows // 2

    def assemble():
        parts = [jnp.zeros((8, LANES), jnp.float32) for _ in range(6)]
        spot = lax.broadcasted_iota(jnp.int32, (8, LANES), 1)
        for i in range(16):
            row, shift = divmod(i * width, LANES)
            x = jnp.concatenate([norm_all[i % 8 * n_rows + 2 * g + i // 8] for g in range(8)], axis=0)
            x = pltpu.roll(x, shift, 1) if shift else x
            first = (spot >= shift) & (spot < shift + width)
            parts[row] = jnp.where(first, x, parts[row])
            if shift + width > LANES:
                parts[row + 1] = jnp.where(spot < shift + width - LANES, x, parts[row + 1])
        for g in range(8):
            for row in range(5):
                norm_lines[5 * g + row : 5 * g + row + 1, :] = parts[row][g : g + 1, :]
        norm_line[...] = norm_lines[...].astype(jnp.bfloat16)

    def norm_step(half):
        for q in range(2):
            @pl.when((half > 0) & (half <= reach[q]))
            def _():
                norm_turn(q, half).wait()

            @pl.when(half < reach[q])
            def _():
                norm_turn(q, half + 1).start()

        @pl.when(gateway & (half == meet))
        def _():
            norm_twin.start()

        @pl.when(gateway & (half == meet + 1))
        def _():
            norm_twin.wait()
            norm_up.start()
            norm_down.start()

        @pl.when(gateway & (half == meet + 2))
        def _():
            norm_up.wait()
            norm_down.wait()
            norm_far.start()

        @pl.when(gateway & (half == meet + 3))
        def _():
            norm_far.wait()
            assemble()

        for q in range(2):
            @pl.when(half == meet + 4 + far[q])
            def _():
                pl.when(takes[q])(lambda: norm_pass(q).wait_recv())
                pl.when(passes[q])(lambda: norm_pass(q).start())

    small[0].wait()
    low = low_buf[...].T
    small[1].wait()
    before = None
    for c in order:
        delta = jnp.dot(low, high_buf[:, c * LANES:(c + 1) * LANES], preferred_element_type=jnp.float32)
        loads[c].wait()
        mine_ref[c] = (train_buf[c].astype(jnp.float32) + mix_rate * delta).astype(jnp.bfloat16)
        if c == order[1]:
            pl.semaphore_wait(barrier, jnp.where(gateway, 7, 4))
        if before is not None:
            ring_copy(before, me, after[before // per_ring], 0, True).start()
        before = c
    small[2].wait()
    small[3].wait()
    norm_all[slot, :, :] = jnp.zeros((1, LANES), jnp.float32)
    norm_all[slot, :, 0:width] = norm_buf[0] + norm_buf[1]
    ring_copy(before, me, after[before // per_ring], 0, True).start()

    for c in order:
        turn(c, me, True)

    def arrived(hop, forward):
        for i, c in enumerate(order):
            q = c // per_ring
            origin = ring_device(q // 2, (pos[q] + (n_rows - way[q]) * hop) % n_rows)
            ring_copy(c, origin, after[q], hop - 1).wait_recv()
            ring_copy(c, me, after[q], 0, True).wait_send()
            if forward:
                ring_copy(c, origin, after[q], hop).start()
            turn(c, origin)
            if forward and (i + 1) % (chunks // 2) == 0:
                norm_step(2 * (hop - 1) + (i + 1) // (chunks // 2) - 1)

    def body(hop, carry):
        arrived(hop, True)
        return carry

    lax.fori_loop(1, steps, body, 0)
    norm_step(2 * (steps - 1))

    for q in range(2):
        pl.when(passes[q])(lambda: norm_pass(q).wait_send())
    norm_out_ref[...] = norm_line[...]
    arrived(steps, False)


def scoped_kernel(n_rows, n_tp, depth, chunks, per_ring, *refs):
    sem = pltpu.SemaphoreType.DMA
    pl.run_scoped(
        functools.partial(kernel, n_rows, n_tp, depth, chunks, per_ring, *refs),
        sem((4,)), sem((chunks,)), sem((chunks,)), sem((n_rows - 1, chunks)),
        sem((4,)), sem((4,)), sem((2, n_rows // 2)), sem((2, n_rows // 2)), sem((2,)), sem((2,)),
    )


def late_place(n_rows, q, me, away):
    position, way = ring_position(q // 2, me), 1 if q % 2 == 0 else n_rows - 1
    origin = ring_device(q // 2, (position + way * away) % n_rows)
    other = origin + 1 - 2 * (origin % 2)
    gap = (ring_position(q // 2, other) + n_rows - position) * way % n_rows
    return origin, gap


def late_kernel(
    n_rows, depth, chunks, per_ring, first_ref, mine_ref, patch_ref, late, stash, send_sem, recv_sem, stash_sem
):
    me = lax.axis_index("rows")
    my_tp = lax.axis_index("tp")
    count = splits(my_tp)
    order = [q * per_ring + k for k in range(per_ring) for q in range(4)]

    def neighbour(q, step):
        way = 1 if q % 2 == 0 else n_rows - 1
        return ring_device(q // 2, (ring_position(q // 2, me) + step * way) % n_rows)

    def late_copy(c, hop, first):
        q = c // per_ring
        return pltpu.make_async_remote_copy(
            src_ref=mine_ref.at[c] if first else late.at[hop - 1, c],
            dst_ref=late.at[hop, c],
            send_sem=send_sem.at[c],
            recv_sem=recv_sem.at[hop, c],
            device_id=(neighbour(q, n_rows - 1), my_tp),
            device_id_type=MESH,
        )

    def stash_copy(q, slot):
        origin, _ = late_place(n_rows, q, me, slot + 1)
        rows = pl.ds(q * per_ring * LANES, per_ring * LANES)
        lanes = pl.ds(pl.multiple_of(origin // 2 * 2 * depth + 256, LANES), LANES)
        return pltpu.make_async_copy(first_ref.at[rows, lanes], stash.at[slot, rows, :], stash_sem.at[slot, q])

    def turn(c, slot):
        q = c // per_ring
        origin, gap = late_place(n_rows, q, me, slot + 1)
        odd = origin % 2
        rows = pl.ds(c * LANES, LANES)
        main = late[slot, c, pl.ds(pl.multiple_of(odd * 64, 64), 256), :]
        patch_ref[slot, rows, 0:256] = main.T
        rest = late[slot, c, pl.ds(pl.multiple_of((1 - odd) * 256, 64), 64), :]
        shared = patch_ref.at[slot, rows, 256:384]
        put_half(shared, jnp.concatenate([rest, rest], axis=0).T, odd)

        @pl.when((gap == 0) | (gap > count))
        def _():
            put_half(shared, stash[slot, rows, :], 1 - odd)

        @pl.when((gap > 0) & (gap <= slot))
        def _():
            put_half(shared, patch_ref[gap - 1, rows, 256:384], 1 - odd)

    barrier = pltpu.get_barrier_semaphore()
    for q in range(4):
        pl.semaphore_signal(barrier, inc=1, device_id=(neighbour(q, 1), my_tp), device_id_type=MESH)
    pl.semaphore_wait(barrier, 4)
    for c in order:
        late_copy(c, 0, True).start()
    for slot in range(SPLIT):
        @pl.when(slot < count)
        def _():
            for q in range(4):
                stash_copy(q, slot).start()
    for slot in range(SPLIT):
        @pl.when(slot < count)
        def _():
            for q in range(4):
                stash_copy(q, slot).wait()
    for hop in range(SPLIT):
        @pl.when(hop < count)
        def _():
            for c in order:
                late_copy(c, hop, hop == 0).wait()
                if hop + 1 < SPLIT:
                    pl.when(hop + 1 < count)(lambda: late_copy(c, hop + 1, False).start())
                turn(c, hop)


def scoped_late_kernel(n_rows, depth, chunks, per_ring, *refs):
    sem = pltpu.SemaphoreType.DMA
    pl.run_scoped(
        functools.partial(late_kernel, n_rows, depth, chunks, per_ring, *refs),
        sem((chunks,)), sem((SPLIT, chunks)), sem((SPLIT, 4)),
    )


def write_kernel(pieces, held_ref, norm_ref, out_ref, norm_out_ref, sems):
    rows = held_ref.shape[0] // pieces
    copies = []
    for i in range(pieces):
        part = pl.ds(i * rows, rows)
        copies.append(pltpu.make_async_copy(held_ref.at[part, :], out_ref.at[part, :], sems.at[i]))
        copies[-1].start()
    copies.append(pltpu.make_async_copy(norm_ref, norm_out_ref, sems.at[pieces]))
    copies[-1].start()
    for copy in copies:
        copy.wait()


def patch_kernel(n_rows, depth, quarter, patch_ref, first_ref, out_ref, main_sem, shared_sem):
    me = lax.axis_index("rows")
    count = splits(lax.axis_index("tp"))

    def copies(q, slot):
        origin, gap = late_place(n_rows, q, me, slot + 1)
        base = origin // 2 * 2 * depth
        rows = pl.ds(q * quarter, quarter)
        lanes = pl.ds(pl.multiple_of(base + origin % 2 * 384, LANES), 256)
        shared_lanes = pl.ds(pl.multiple_of(base + 256, LANES), LANES)
        main = pltpu.make_async_copy(patch_ref.at[slot, rows, 0:256], out_ref.at[rows, lanes], main_sem.at[slot, q])
        shared = pltpu.make_async_copy(
            patch_ref.at[slot, rows, 256:384], out_ref.at[rows, shared_lanes], shared_sem.at[slot, q])
        return main, shared, (gap <= slot) | (gap > count)

    for slot in range(SPLIT):
        @pl.when(slot < count)
        def _():
            for main, shared, last in [copies(q, slot) for q in range(4)]:
                main.start()
                pl.when(last)(shared.start)
    for slot in range(SPLIT):
        @pl.when(slot < count)
        def _():
            for main, shared, last in [copies(q, slot) for q in range(4)]:
                main.wait()
                pl.when(last)(shared.wait)


def per_device(train_up, low_up, high_up, norm_train, norm_step):
    n_rows, n_tp = lax.axis_size("rows"), lax.axis_size("tp")
    depth, width = train_up.shape
    rank, own = low_up.shape[1], norm_train.shape[0]
    chunks = width // LANES
    per_ring = chunks // 4
    norm_shape = (n_rows * n_tp * own // LANES, LANES)
    anywhere, vmem = pl.BlockSpec(memory_space=pl.ANY), pl.BlockSpec(memory_space=pltpu.VMEM)
    held, mine, norm = pl.pallas_call(
        functools.partial(scoped_kernel, n_rows, n_tp, depth, chunks, per_ring),
        out_shape=(
            pltpu.VMEM((width, n_rows * depth), jnp.bfloat16),
            pltpu.VMEM((chunks, depth, LANES), jnp.bfloat16),
            pltpu.VMEM(norm_shape, jnp.bfloat16),
        ),
        in_specs=[anywhere] * 5,
        out_specs=(vmem, vmem, vmem),
        scratch_shapes=[
            pltpu.VMEM((chunks, depth, LANES), jnp.bfloat16),
            pltpu.VMEM((rank, depth), jnp.bfloat16),
            pltpu.VMEM((rank, width), jnp.bfloat16),
            pltpu.VMEM((2, 1, own), jnp.float32),
            pltpu.VMEM((chunks, n_rows * depth, LANES), jnp.bfloat16),
            pltpu.VMEM((n_rows * n_tp, 1, LANES), jnp.float32),
            pltpu.VMEM(norm_shape, jnp.float32),
            pltpu.VMEM(norm_shape, jnp.bfloat16),
        ],
        compiler_params=pltpu.CompilerParams(
            collective_id=0, has_side_effects=True, vmem_limit_bytes=30 * 1024 * 1024
        ),
    )(train_up, low_up.T, high_up, norm_train.reshape(1, -1), norm_step.reshape(1, -1))
    pieces = 16
    first, norm = pl.pallas_call(
        functools.partial(write_kernel, pieces),
        out_shape=(
            jax.ShapeDtypeStruct(held.shape, held.dtype),
            jax.ShapeDtypeStruct(norm_shape, jnp.bfloat16),
        ),
        in_specs=[anywhere, anywhere],
        out_specs=(anywhere, anywhere),
        scratch_shapes=[pltpu.SemaphoreType.DMA((pieces + 1,))],
        compiler_params=pltpu.CompilerParams(vmem_limit_bytes=1024 * 1024),
    )(held, norm)
    patch = pl.pallas_call(
        functools.partial(scoped_late_kernel, n_rows, depth, chunks, per_ring),
        out_shape=pltpu.VMEM((SPLIT, width, 384), jnp.bfloat16),
        in_specs=[anywhere, vmem],
        out_specs=vmem,
        scratch_shapes=[
            pltpu.VMEM((SPLIT, chunks, depth, LANES), jnp.bfloat16),
            pltpu.VMEM((SPLIT, width, LANES), jnp.bfloat16),
        ],
        compiler_params=pltpu.CompilerParams(
            collective_id=1, has_side_effects=True, vmem_limit_bytes=40 * 1024 * 1024
        ),
    )(first, mine)
    ready = pl.pallas_call(
        functools.partial(patch_kernel, n_rows, depth, width // 4),
        out_shape=jax.ShapeDtypeStruct(held.shape, held.dtype),
        in_specs=[anywhere, anywhere],
        out_specs=anywhere,
        input_output_aliases={1: 0},
        scratch_shapes=[pltpu.SemaphoreType.DMA((SPLIT, 4)), pltpu.SemaphoreType.DMA((SPLIT, 4))],
        compiler_params=pltpu.CompilerParams(vmem_limit_bytes=1024 * 1024),
    )(patch, first)
    return ready, norm.reshape(-1)


def solution(mesh):
    placed = (P("rows", "tp"), P("rows", None), P(None, "tp"), P(("rows", "tp")), P(("rows", "tp")))
    return jax.shard_map(
        per_device, mesh=mesh, in_specs=placed, out_specs=(P("tp", None), P()), check_vma=False
    )
```

```python
import functools

import jax
import jax.numpy as jnp
from jax import lax
from jax.experimental import pallas as pl
from jax.experimental.pallas import tpu as pltpu
from jax.sharding import PartitionSpec as P

mix_rate = 2.0
MESH = pl.DeviceIdType.MESH
SPLIT = 4
SIDE = 4
LANES = 128


def ring_position(cycle, device):
    y, x = device // SIDE, device % SIDE
    return SIDE * (y if cycle == 0 else x) + (x + y) % SIDE


def ring_device(cycle, position):
    a = position // SIDE
    b = (position % SIDE + SIDE - a) % SIDE
    return SIDE * a + b if cycle == 0 else SIDE * b + a


def put_half(tile, value, half):
    @pl.when(half == 0)
    def _():
        tile[:, :64] = value[:, :64]

    @pl.when(half == 1)
    def _():
        tile[:, 64:] = value[:, 64:]


def splits(tp):
    return 1 + (SPLIT - 1) * (tp % 2)


def kernel(
    n_rows, n_tp, depth, chunks, per_ring,
    train_ref, low_ref, high_ref, normt_ref, norms_ref,
    out_ref, mine_ref, norm_out_ref,
    train_buf, low_buf, high_buf, norm_buf, held, norm_all, norm_lines, norm_line,
    small_sem, load_sem, send_sem, recv_sem, norm_send, norm_recv, turn_send, turn_recv, line_send, line_recv,
):
    me = lax.axis_index("rows")
    my_tp = lax.axis_index("tp")
    steps = n_rows - 1 - splits(my_tp)
    pos = [ring_position(q // 2, me) for q in range(4)]
    way = [1 if q % 2 == 0 else n_rows - 1 for q in range(4)]
    after = [ring_device(q // 2, (pos[q] + way[q]) % n_rows) for q in range(4)]
    twin = my_tp + 1 - 2 * (my_tp % 2)
    up, down = (my_tp + 2) % n_tp, (my_tp + n_tp - 2) % n_tp

    barrier = pltpu.get_barrier_semaphore()
    for q in range(4):
        pl.semaphore_signal(barrier, inc=1, device_id=(after[q], my_tp), device_id_type=MESH)
    gateway = me == 0

    @pl.when(gateway)
    def _():
        for other in (twin, up, down):
            pl.semaphore_signal(barrier, inc=1, device_id=(me, other), device_id_type=MESH)

    order = [q * per_ring + k for k in range(per_ring) for q in range(4)]
    small = [
        pltpu.make_async_copy(low_ref, low_buf, small_sem.at[0]),
        pltpu.make_async_copy(high_ref, high_buf, small_sem.at[1]),
        pltpu.make_async_copy(normt_ref, norm_buf.at[0], small_sem.at[2]),
        pltpu.make_async_copy(norms_ref, norm_buf.at[1], small_sem.at[3]),
    ]
    loads = [
        pltpu.make_async_copy(train_ref.at[:, pl.ds(c * LANES, LANES)], train_buf.at[c], load_sem.at[c])
        for c in range(chunks)
    ]
    for load in small:
        load.start()
    for c in order:
        loads[c].start()

    def ring_copy(c, origin, to, hop, first=False):
        rows = pl.ds(pl.multiple_of(origin * depth, 64), depth)
        return pltpu.make_async_remote_copy(
            src_ref=mine_ref.at[c] if first else held.at[c, rows, :],
            dst_ref=held.at[c, rows, :],
            send_sem=send_sem.at[c],
            recv_sem=recv_sem.at[hop, c],
            device_id=(to, my_tp),
            device_id_type=MESH,
        )

    def turn(c, origin, first=False):
        pair, odd = origin // 2, origin % 2
        base = pl.multiple_of(pair * 2 * depth, LANES)
        top = 0 if first else origin * depth
        source = mine_ref if first else held
        main = source[c, pl.ds(pl.multiple_of(top + odd * 64, 64), 256), :]
        out_ref[pl.ds(c * LANES, LANES), pl.ds(pl.multiple_of(base + odd * 384, LANES), 256)] = main.T
        rest = source[c, pl.ds(pl.multiple_of(top + (1 - odd) * 256, 64), 64), :]
        rest = jnp.concatenate([rest, rest], axis=0).T
        shared = out_ref.at[pl.ds(c * LANES, LANES), pl.ds(pl.multiple_of(base + 256, LANES), LANES)]
        put_half(shared, rest, odd)

    slot = my_tp * n_rows + me
    width = normt_ref.shape[1]

    def norm_copy(i, first, count, other):
        part = pl.ds(first * n_rows, count * n_rows)
        return pltpu.make_async_remote_copy(
            src_ref=norm_all.at[part], dst_ref=norm_all.at[part],
            send_sem=norm_send.at[i], recv_sem=norm_recv.at[i],
            device_id=(me, other), device_id_type=MESH)

    norm_twin = norm_copy(0, my_tp, 1, twin)
    norm_up = norm_copy(1, my_tp // 2 * 2, 2, up)
    norm_down = norm_copy(2, my_tp // 2 * 2, 2, down)
    norm_far = norm_copy(3, down // 2 * 2, 2, up)

    def norm_turn(q, hop):
        origin = ring_device(0, (pos[q] + (n_rows - way[q]) * (hop - 1)) % n_rows)
        part = pl.ds(my_tp * n_rows + origin, 1)
        return pltpu.make_async_remote_copy(
            src_ref=norm_all.at[part], dst_ref=norm_all.at[part],
            send_sem=turn_send.at[q, hop - 1], recv_sem=turn_recv.at[q, hop - 1],
            device_id=(after[q], my_tp), device_id_type=MESH)

    def norm_pass(q):
        return pltpu.make_async_remote_copy(
            src_ref=norm_line, dst_ref=norm_line, send_sem=line_send.at[q], recv_sem=line_recv.at[q],
            device_id=(after[q], my_tp), device_id_type=MESH)

    reach = (n_rows // 2, (n_rows - 1) // 2)
    far = (pos[0], (n_rows - pos[0]) % n_rows)
    passes = [far[q] < reach[q] for q in range(2)]
    takes = [(far[q] > 0) & (far[q] <= reach[q]) for q in range(2)]
    meet = n_rows // 2

    def assemble():
        parts = [jnp.zeros((8, LANES), jnp.float32) for _ in range(6)]
        spot = lax.broadcasted_iota(jnp.int32, (8, LANES), 1)
        for i in range(16):
            row, shift = divmod(i * width, LANES)
            x = jnp.concatenate([norm_all[i % 8 * n_rows + 2 * g + i // 8] for g in range(8)], axis=0)
            x = pltpu.roll(x, shift, 1) if shift else x
            first = (spot >= shift) & (spot < shift + width)
            parts[row] = jnp.where(first, x, parts[row])
            if shift + width > LANES:
                parts[row + 1] = jnp.where(spot < shift + width - LANES, x, parts[row + 1])
        for g in range(8):
            for row in range(5):
                norm_lines[5 * g + row : 5 * g + row + 1, :] = parts[row][g : g + 1, :]
        norm_line[...] = norm_lines[...].astype(jnp.bfloat16)

    def norm_step(half):
        for q in range(2):
            @pl.when((half > 0) & (half <= reach[q]))
            def _():
                norm_turn(q, half).wait()

            @pl.when(half < reach[q])
            def _():
                norm_turn(q, half + 1).start()

        @pl.when(gateway & (half == meet))
        def _():
            norm_twin.start()

        @pl.when(gateway & (half == meet + 1))
        def _():
            norm_twin.wait()
            norm_up.start()
            norm_down.start()

        @pl.when(gateway & (half == meet + 2))
        def _():
            norm_up.wait()
            norm_down.wait()
            norm_far.start()

        @pl.when(gateway & (half == meet + 3))
        def _():
            norm_far.wait()
            assemble()

        for q in range(2):
            @pl.when(half == meet + 4 + far[q])
            def _():
                pl.when(takes[q])(lambda: norm_pass(q).wait_recv())
                pl.when(passes[q])(lambda: norm_pass(q).start())

    small[0].wait()
    low = low_buf[...].T
    small[1].wait()
    before = None
    for c in order:
        delta = jnp.dot(low, high_buf[:, c * LANES:(c + 1) * LANES], preferred_element_type=jnp.float32)
        loads[c].wait()
        mine_ref[c] = (train_buf[c].astype(jnp.float32) + mix_rate * delta).astype(jnp.bfloat16)
        if c == order[1]:
            pl.semaphore_wait(barrier, jnp.where(gateway, 7, 4))
        if before is not None:
            ring_copy(before, me, after[before // per_ring], 0, True).start()
        before = c
    small[2].wait()
    small[3].wait()
    norm_all[slot, :, :] = jnp.zeros((1, LANES), jnp.float32)
    norm_all[slot, :, 0:width] = norm_buf[0] + norm_buf[1]

    for i, c in enumerate(order):
        turn(c, me, True)
        if i == 0:
            ring_copy(before, me, after[before // per_ring], 0, True).start()

    def arrived(hop, forward):
        for i, c in enumerate(order):
            q = c // per_ring
            origin = ring_device(q // 2, (pos[q] + (n_rows - way[q]) * hop) % n_rows)
            ring_copy(c, origin, after[q], hop - 1).wait_recv()
            ring_copy(c, me, after[q], 0, True).wait_send()
            if forward:
                ring_copy(c, origin, after[q], hop).start()
            turn(c, origin)
            if forward and (i + 1) % (chunks // 2) == 0:
                norm_step(2 * (hop - 1) + (i + 1) // (chunks // 2) - 1)

    def body(hop, carry):
        arrived(hop, True)
        return carry

    lax.fori_loop(1, steps, body, 0)
    norm_step(2 * (steps - 1))

    for q in range(2):
        pl.when(passes[q])(lambda: norm_pass(q).wait_send())
    norm_out_ref[...] = norm_line[...]
    arrived(steps, False)


def scoped_kernel(n_rows, n_tp, depth, chunks, per_ring, *refs):
    sem = pltpu.SemaphoreType.DMA
    pl.run_scoped(
        functools.partial(kernel, n_rows, n_tp, depth, chunks, per_ring, *refs),
        sem((4,)), sem((chunks,)), sem((chunks,)), sem((n_rows - 1, chunks)),
        sem((4,)), sem((4,)), sem((2, n_rows // 2)), sem((2, n_rows // 2)), sem((2,)), sem((2,)),
    )


def late_place(n_rows, q, me, away):
    position, way = ring_position(q // 2, me), 1 if q % 2 == 0 else n_rows - 1
    origin = ring_device(q // 2, (position + way * away) % n_rows)
    other = origin + 1 - 2 * (origin % 2)
    gap = (ring_position(q // 2, other) + n_rows - position) * way % n_rows
    return origin, gap


def late_kernel(
    n_rows, depth, chunks, per_ring, first_ref, mine_ref, patch_ref, late, stash, send_sem, recv_sem, stash_sem
):
    me = lax.axis_index("rows")
    my_tp = lax.axis_index("tp")
    count = splits(my_tp)
    order = [q * per_ring + k for k in range(per_ring) for q in range(4)]

    def neighbour(q, step):
        way = 1 if q % 2 == 0 else n_rows - 1
        return ring_device(q // 2, (ring_position(q // 2, me) + step * way) % n_rows)

    def late_copy(c, hop, first):
        q = c // per_ring
        return pltpu.make_async_remote_copy(
            src_ref=mine_ref.at[c] if first else late.at[hop - 1, c],
            dst_ref=late.at[hop, c],
            send_sem=send_sem.at[c],
            recv_sem=recv_sem.at[hop, c],
            device_id=(neighbour(q, n_rows - 1), my_tp),
            device_id_type=MESH,
        )

    def stash_copy(q, slot):
        origin, _ = late_place(n_rows, q, me, slot + 1)
        rows = pl.ds(q * per_ring * LANES, per_ring * LANES)
        lanes = pl.ds(pl.multiple_of(origin // 2 * 2 * depth + 256, LANES), LANES)
        return pltpu.make_async_copy(first_ref.at[rows, lanes], stash.at[slot, rows, :], stash_sem.at[slot, q])

    def turn(c, slot):
        q = c // per_ring
        origin, gap = late_place(n_rows, q, me, slot + 1)
        odd = origin % 2
        rows = pl.ds(c * LANES, LANES)
        main = late[slot, c, pl.ds(pl.multiple_of(odd * 64, 64), 256), :]
        patch_ref[slot, rows, 0:256] = main.T
        rest = late[slot, c, pl.ds(pl.multiple_of((1 - odd) * 256, 64), 64), :]
        shared = patch_ref.at[slot, rows, 256:384]
        put_half(shared, jnp.concatenate([rest, rest], axis=0).T, odd)

        @pl.when((gap == 0) | (gap > count))
        def _():
            put_half(shared, stash[slot, rows, :], 1 - odd)

        @pl.when((gap > 0) & (gap <= slot))
        def _():
            put_half(shared, patch_ref[gap - 1, rows, 256:384], 1 - odd)

    barrier = pltpu.get_barrier_semaphore()
    for q in range(4):
        pl.semaphore_signal(barrier, inc=1, device_id=(neighbour(q, 1), my_tp), device_id_type=MESH)
    pl.semaphore_wait(barrier, 4)
    for c in order:
        late_copy(c, 0, True).start()
    for slot in range(SPLIT):
        @pl.when(slot < count)
        def _():
            for q in range(4):
                stash_copy(q, slot).start()
    for slot in range(SPLIT):
        @pl.when(slot < count)
        def _():
            for q in range(4):
                stash_copy(q, slot).wait()
    for hop in range(SPLIT):
        @pl.when(hop < count)
        def _():
            for c in order:
                late_copy(c, hop, hop == 0).wait()
                if hop + 1 < SPLIT:
                    pl.when(hop + 1 < count)(lambda: late_copy(c, hop + 1, False).start())
                turn(c, hop)


def scoped_late_kernel(n_rows, depth, chunks, per_ring, *refs):
    sem = pltpu.SemaphoreType.DMA
    pl.run_scoped(
        functools.partial(late_kernel, n_rows, depth, chunks, per_ring, *refs),
        sem((chunks,)), sem((SPLIT, chunks)), sem((SPLIT, 4)),
    )


def write_kernel(pieces, held_ref, norm_ref, out_ref, norm_out_ref, sems):
    rows = held_ref.shape[0] // pieces
    copies = []
    for i in range(pieces):
        part = pl.ds(i * rows, rows)
        copies.append(pltpu.make_async_copy(held_ref.at[part, :], out_ref.at[part, :], sems.at[i]))
        copies[-1].start()
    copies.append(pltpu.make_async_copy(norm_ref, norm_out_ref, sems.at[pieces]))
    copies[-1].start()
    for copy in copies:
        copy.wait()


def patch_kernel(n_rows, depth, quarter, patch_ref, first_ref, out_ref, main_sem, shared_sem):
    me = lax.axis_index("rows")
    count = splits(lax.axis_index("tp"))

    def copies(q, slot):
        origin, gap = late_place(n_rows, q, me, slot + 1)
        base = origin // 2 * 2 * depth
        rows = pl.ds(q * quarter, quarter)
        lanes = pl.ds(pl.multiple_of(base + origin % 2 * 384, LANES), 256)
        shared_lanes = pl.ds(pl.multiple_of(base + 256, LANES), LANES)
        main = pltpu.make_async_copy(patch_ref.at[slot, rows, 0:256], out_ref.at[rows, lanes], main_sem.at[slot, q])
        shared = pltpu.make_async_copy(
            patch_ref.at[slot, rows, 256:384], out_ref.at[rows, shared_lanes], shared_sem.at[slot, q])
        return main, shared, (gap <= slot) | (gap > count)

    for slot in range(SPLIT):
        @pl.when(slot < count)
        def _():
            for main, shared, last in [copies(q, slot) for q in range(4)]:
                main.start()
                pl.when(last)(shared.start)
    for slot in range(SPLIT):
        @pl.when(slot < count)
        def _():
            for main, shared, last in [copies(q, slot) for q in range(4)]:
                main.wait()
                pl.when(last)(shared.wait)


def per_device(train_up, low_up, high_up, norm_train, norm_step):
    n_rows, n_tp = lax.axis_size("rows"), lax.axis_size("tp")
    depth, width = train_up.shape
    rank, own = low_up.shape[1], norm_train.shape[0]
    chunks = width // LANES
    per_ring = chunks // 4
    norm_shape = (n_rows * n_tp * own // LANES, LANES)
    anywhere, vmem = pl.BlockSpec(memory_space=pl.ANY), pl.BlockSpec(memory_space=pltpu.VMEM)
    held, mine, norm = pl.pallas_call(
        functools.partial(scoped_kernel, n_rows, n_tp, depth, chunks, per_ring),
        out_shape=(
            pltpu.VMEM((width, n_rows * depth), jnp.bfloat16),
            pltpu.VMEM((chunks, depth, LANES), jnp.bfloat16),
            pltpu.VMEM(norm_shape, jnp.bfloat16),
        ),
        in_specs=[anywhere] * 5,
        out_specs=(vmem, vmem, vmem),
        scratch_shapes=[
            pltpu.VMEM((chunks, depth, LANES), jnp.bfloat16),
            pltpu.VMEM((rank, depth), jnp.bfloat16),
            pltpu.VMEM((rank, width), jnp.bfloat16),
            pltpu.VMEM((2, 1, own), jnp.float32),
            pltpu.VMEM((chunks, n_rows * depth, LANES), jnp.bfloat16),
            pltpu.VMEM((n_rows * n_tp, 1, LANES), jnp.float32),
            pltpu.VMEM(norm_shape, jnp.float32),
            pltpu.VMEM(norm_shape, jnp.bfloat16),
        ],
        compiler_params=pltpu.CompilerParams(
            collective_id=0, has_side_effects=True, vmem_limit_bytes=30 * 1024 * 1024
        ),
    )(train_up, low_up.T, high_up, norm_train.reshape(1, -1), norm_step.reshape(1, -1))
    pieces = 16
    first, norm = pl.pallas_call(
        functools.partial(write_kernel, pieces),
        out_shape=(
            jax.ShapeDtypeStruct(held.shape, held.dtype),
            jax.ShapeDtypeStruct(norm_shape, jnp.bfloat16),
        ),
        in_specs=[anywhere, anywhere],
        out_specs=(anywhere, anywhere),
        scratch_shapes=[pltpu.SemaphoreType.DMA((pieces + 1,))],
        compiler_params=pltpu.CompilerParams(vmem_limit_bytes=1024 * 1024),
    )(held, norm)
    patch = pl.pallas_call(
        functools.partial(scoped_late_kernel, n_rows, depth, chunks, per_ring),
        out_shape=pltpu.VMEM((SPLIT, width, 384), jnp.bfloat16),
        in_specs=[anywhere, vmem],
        out_specs=vmem,
        scratch_shapes=[
            pltpu.VMEM((SPLIT, chunks, depth, LANES), jnp.bfloat16),
            pltpu.VMEM((SPLIT, width, LANES), jnp.bfloat16),
        ],
        compiler_params=pltpu.CompilerParams(
            collective_id=1, has_side_effects=True, vmem_limit_bytes=40 * 1024 * 1024
        ),
    )(first, mine)
    ready = pl.pallas_call(
        functools.partial(patch_kernel, n_rows, depth, width // 4),
        out_shape=jax.ShapeDtypeStruct(held.shape, held.dtype),
        in_specs=[anywhere, anywhere],
        out_specs=anywhere,
        input_output_aliases={1: 0},
        scratch_shapes=[pltpu.SemaphoreType.DMA((SPLIT, 4)), pltpu.SemaphoreType.DMA((SPLIT, 4))],
        compiler_params=pltpu.CompilerParams(vmem_limit_bytes=1024 * 1024),
    )(patch, first)
    return ready, norm.reshape(-1)


def solution(mesh):
    placed = (P("rows", "tp"), P("rows", None), P(None, "tp"), P(("rows", "tp")), P(("rows", "tp")))
    return jax.shard_map(
        per_device, mesh=mesh, in_specs=placed, out_specs=(P("tp", None), P()), check_vma=False
    )
```

```python
import functools

import jax
import jax.numpy as jnp
from jax import lax
from jax.experimental import pallas as pl
from jax.experimental.pallas import tpu as pltpu
from jax.sharding import PartitionSpec as P

mix_rate = 2.0
MESH = pl.DeviceIdType.MESH
SPLIT = 4
SIDE = 4
LANES = 128


def ring_position(cycle, device):
    y, x = device // SIDE, device % SIDE
    return SIDE * (y if cycle == 0 else x) + (x + y) % SIDE


def ring_device(cycle, position):
    a = position // SIDE
    b = (position % SIDE + SIDE - a) % SIDE
    return SIDE * a + b if cycle == 0 else SIDE * b + a


def put_half(tile, value, half):
    @pl.when(half == 0)
    def _():
        tile[:, :64] = value[:, :64]

    @pl.when(half == 1)
    def _():
        tile[:, 64:] = value[:, 64:]


def splits(tp):
    return 1 + (SPLIT - 1) * (tp % 2)


def kernel(
    n_rows, n_tp, depth, chunks, per_ring,
    train_ref, low_ref, high_ref, normt_ref, norms_ref,
    out_ref, mine_ref, norm_out_ref,
    train_buf, low_buf, high_buf, norm_buf, held, norm_all, norm_lines, norm_line,
    small_sem, load_sem, send_sem, recv_sem, norm_send, norm_recv, turn_send, turn_recv, line_send, line_recv,
):
    me = lax.axis_index("rows")
    my_tp = lax.axis_index("tp")
    steps = n_rows - 1 - splits(my_tp)
    pos = [ring_position(q // 2, me) for q in range(4)]
    way = [1 if q % 2 == 0 else n_rows - 1 for q in range(4)]
    after = [ring_device(q // 2, (pos[q] + way[q]) % n_rows) for q in range(4)]
    twin = my_tp + 1 - 2 * (my_tp % 2)
    up, down = (my_tp + 2) % n_tp, (my_tp + n_tp - 2) % n_tp

    barrier = pltpu.get_barrier_semaphore()
    for q in range(4):
        pl.semaphore_signal(barrier, inc=1, device_id=(after[q], my_tp), device_id_type=MESH)
    gateway = me == 0

    @pl.when(gateway)
    def _():
        for other in (twin, up, down):
            pl.semaphore_signal(barrier, inc=1, device_id=(me, other), device_id_type=MESH)

    order = [q * per_ring + k for k in range(per_ring) for q in range(4)]
    small = [
        pltpu.make_async_copy(low_ref, low_buf, small_sem.at[0]),
        pltpu.make_async_copy(high_ref, high_buf, small_sem.at[1]),
        pltpu.make_async_copy(normt_ref, norm_buf.at[0], small_sem.at[2]),
        pltpu.make_async_copy(norms_ref, norm_buf.at[1], small_sem.at[3]),
    ]
    loads = [
        pltpu.make_async_copy(train_ref.at[:, pl.ds(c * LANES, LANES)], train_buf.at[c], load_sem.at[c])
        for c in range(chunks)
    ]
    for load in small:
        load.start()
    for c in order:
        loads[c].start()

    def ring_copy(c, origin, to, hop, first=False):
        rows = pl.ds(pl.multiple_of(origin * depth, 64), depth)
        return pltpu.make_async_remote_copy(
            src_ref=mine_ref.at[c] if first else held.at[c, rows, :],
            dst_ref=held.at[c, rows, :],
            send_sem=send_sem.at[c],
            recv_sem=recv_sem.at[hop, c],
            device_id=(to, my_tp),
            device_id_type=MESH,
        )

    def turn(c, origin, first=False):
        pair, odd = origin // 2, origin % 2
        base = pl.multiple_of(pair * 2 * depth, LANES)
        top = 0 if first else origin * depth
        source = mine_ref if first else held
        main = source[c, pl.ds(pl.multiple_of(top + odd * 64, 64), 256), :]
        out_ref[pl.ds(c * LANES, LANES), pl.ds(pl.multiple_of(base + odd * 384, LANES), 256)] = main.T
        rest = source[c, pl.ds(pl.multiple_of(top + (1 - odd) * 256, 64), 64), :]
        rest = jnp.concatenate([rest, rest], axis=0).T
        shared = out_ref.at[pl.ds(c * LANES, LANES), pl.ds(pl.multiple_of(base + 256, LANES), LANES)]
        put_half(shared, rest, odd)

    slot = my_tp * n_rows + me
    width = normt_ref.shape[1]

    def norm_copy(i, first, count, other):
        part = pl.ds(first * n_rows, count * n_rows)
        return pltpu.make_async_remote_copy(
            src_ref=norm_all.at[part], dst_ref=norm_all.at[part],
            send_sem=norm_send.at[i], recv_sem=norm_recv.at[i],
            device_id=(me, other), device_id_type=MESH)

    norm_twin = norm_copy(0, my_tp, 1, twin)
    norm_up = norm_copy(1, my_tp // 2 * 2, 2, up)
    norm_down = norm_copy(2, my_tp // 2 * 2, 2, down)
    norm_far = norm_copy(3, down // 2 * 2, 2, up)

    def norm_turn(q, hop):
        origin = ring_device(0, (pos[q] + (n_rows - way[q]) * (hop - 1)) % n_rows)
        part = pl.ds(my_tp * n_rows + origin, 1)
        return pltpu.make_async_remote_copy(
            src_ref=norm_all.at[part], dst_ref=norm_all.at[part],
            send_sem=turn_send.at[q, hop - 1], recv_sem=turn_recv.at[q, hop - 1],
            device_id=(after[q], my_tp), device_id_type=MESH)

    def norm_pass(q):
        return pltpu.make_async_remote_copy(
            src_ref=norm_line, dst_ref=norm_line, send_sem=line_send.at[q], recv_sem=line_recv.at[q],
            device_id=(after[q], my_tp), device_id_type=MESH)

    reach = (n_rows // 2, (n_rows - 1) // 2)
    far = (pos[0], (n_rows - pos[0]) % n_rows)
    passes = [far[q] < reach[q] for q in range(2)]
    takes = [(far[q] > 0) & (far[q] <= reach[q]) for q in range(2)]
    meet = n_rows // 2

    def assemble():
        parts = [jnp.zeros((8, LANES), jnp.float32) for _ in range(6)]
        spot = lax.broadcasted_iota(jnp.int32, (8, LANES), 1)
        for i in range(16):
            row, shift = divmod(i * width, LANES)
            x = jnp.concatenate([norm_all[i % 8 * n_rows + 2 * g + i // 8] for g in range(8)], axis=0)
            x = pltpu.roll(x, shift, 1) if shift else x
            first = (spot >= shift) & (spot < shift + width)
            parts[row] = jnp.where(first, x, parts[row])
            if shift + width > LANES:
                parts[row + 1] = jnp.where(spot < shift + width - LANES, x, parts[row + 1])
        for g in range(8):
            for row in range(5):
                norm_lines[5 * g + row : 5 * g + row + 1, :] = parts[row][g : g + 1, :]
        norm_line[...] = norm_lines[...].astype(jnp.bfloat16)

    def norm_step(half):
        for q in range(2):
            @pl.when((half > 0) & (half <= reach[q]))
            def _():
                norm_turn(q, half).wait()

            @pl.when(half < reach[q])
            def _():
                norm_turn(q, half + 1).start()

        @pl.when(gateway & (half == meet))
        def _():
            norm_twin.start()

        @pl.when(gateway & (half == meet + 1))
        def _():
            norm_twin.wait()
            norm_up.start()
            norm_down.start()

        @pl.when(gateway & (half == meet + 2))
        def _():
            norm_up.wait()
            norm_down.wait()
            norm_far.start()

        @pl.when(gateway & (half == meet + 3))
        def _():
            norm_far.wait()
            assemble()

        for q in range(2):
            @pl.when(half == meet + 4 + far[q])
            def _():
                pl.when(takes[q])(lambda: norm_pass(q).wait_recv())
                pl.when(passes[q])(lambda: norm_pass(q).start())

    small[0].wait()
    low = low_buf[...].T
    small[1].wait()
    before = None
    for c in order:
        delta = jnp.dot(low, high_buf[:, c * LANES:(c + 1) * LANES], preferred_element_type=jnp.float32)
        loads[c].wait()
        mine_ref[c] = (train_buf[c].astype(jnp.float32) + mix_rate * delta).astype(jnp.bfloat16)
        if c == order[1]:
            pl.semaphore_wait(barrier, jnp.where(gateway, 7, 4))
        if before is not None:
            ring_copy(before, me, after[before // per_ring], 0, True).start()
        before = c
    small[2].wait()
    small[3].wait()
    norm_all[slot, :, :] = jnp.zeros((1, LANES), jnp.float32)
    norm_all[slot, :, 0:width] = norm_buf[0] + norm_buf[1]

    for i, c in enumerate(order):
        turn(c, me, True)
        if i == 0:
            ring_copy(before, me, after[before // per_ring], 0, True).start()

    def arrived(hop, forward):
        for i, c in enumerate(order):
            q = c // per_ring
            origin = ring_device(q // 2, (pos[q] + (n_rows - way[q]) * hop) % n_rows)
            ring_copy(c, origin, after[q], hop - 1).wait_recv()
            ring_copy(c, me, after[q], 0, True).wait_send()
            if forward:
                ring_copy(c, origin, after[q], hop).start()
            turn(c, origin)
            if forward and (i + 1) % (chunks // 2) == 0:
                norm_step(2 * (hop - 1) + (i + 1) // (chunks // 2) - 1)

    def body(hop, carry):
        arrived(hop, True)
        return carry

    lax.fori_loop(1, steps, body, 0)
    norm_step(2 * (steps - 1))

    for q in range(2):
        pl.when(passes[q])(lambda: norm_pass(q).wait_send())
    norm_out_ref[...] = norm_line[...]
    arrived(steps, False)


def scoped_kernel(n_rows, n_tp, depth, chunks, per_ring, *refs):
    sem = pltpu.SemaphoreType.DMA
    pl.run_scoped(
        functools.partial(kernel, n_rows, n_tp, depth, chunks, per_ring, *refs),
        sem((4,)), sem((chunks,)), sem((chunks,)), sem((n_rows - 1, chunks)),
        sem((4,)), sem((4,)), sem((2, n_rows // 2)), sem((2, n_rows // 2)), sem((2,)), sem((2,)),
    )


def late_place(n_rows, q, me, away):
    position, way = ring_position(q // 2, me), 1 if q % 2 == 0 else n_rows - 1
    origin = ring_device(q // 2, (position + way * away) % n_rows)
    other = origin + 1 - 2 * (origin % 2)
    gap = (ring_position(q // 2, other) + n_rows - position) * way % n_rows
    return origin, gap


def late_kernel(
    n_rows, depth, chunks, per_ring, first_ref, mine_ref, patch_ref, late, stash, send_sem, recv_sem, stash_sem
):
    me = lax.axis_index("rows")
    my_tp = lax.axis_index("tp")
    count = splits(my_tp)
    order = [q * per_ring + k for k in range(per_ring) for q in range(4)]

    def neighbour(q, step):
        way = 1 if q % 2 == 0 else n_rows - 1
        return ring_device(q // 2, (ring_position(q // 2, me) + step * way) % n_rows)

    def late_copy(c, hop, first):
        q = c // per_ring
        return pltpu.make_async_remote_copy(
            src_ref=mine_ref.at[c] if first else late.at[hop - 1, c],
            dst_ref=late.at[hop, c],
            send_sem=send_sem.at[c],
            recv_sem=recv_sem.at[hop, c],
            device_id=(neighbour(q, n_rows - 1), my_tp),
            device_id_type=MESH,
        )

    def stash_copy(q, slot):
        origin, _ = late_place(n_rows, q, me, slot + 1)
        rows = pl.ds(q * per_ring * LANES, per_ring * LANES)
        lanes = pl.ds(pl.multiple_of(origin // 2 * 2 * depth + 256, LANES), LANES)
        return pltpu.make_async_copy(first_ref.at[rows, lanes], stash.at[slot, rows, :], stash_sem.at[slot, q])

    def turn(c, slot):
        q = c // per_ring
        origin, gap = late_place(n_rows, q, me, slot + 1)
        odd = origin % 2
        rows = pl.ds(c * LANES, LANES)
        main = late[slot, c, pl.ds(pl.multiple_of(odd * 64, 64), 256), :]
        patch_ref[slot, rows, pl.ds(pl.multiple_of(odd * LANES, LANES), 256)] = main.T
        rest = late[slot, c, pl.ds(pl.multiple_of((1 - odd) * 256, 64), 64), :]
        shared = patch_ref.at[slot, rows, pl.ds(pl.multiple_of((1 - odd) * 256, LANES), LANES)]
        put_half(shared, jnp.concatenate([rest, rest], axis=0).T, odd)

        @pl.when((gap == 0) | (gap > count))
        def _():
            put_half(shared, stash[slot, rows, :], 1 - odd)

        @pl.when((gap > 0) & (gap <= slot))
        def _():
            put_half(shared, patch_ref[gap - 1, rows, pl.ds(pl.multiple_of(odd * 256, LANES), LANES)], 1 - odd)

    barrier = pltpu.get_barrier_semaphore()
    for q in range(4):
        pl.semaphore_signal(barrier, inc=1, device_id=(neighbour(q, 1), my_tp), device_id_type=MESH)
    pl.semaphore_wait(barrier, 4)
    for c in order:
        late_copy(c, 0, True).start()
    for slot in range(SPLIT):
        @pl.when(slot < count)
        def _():
            for q in range(4):
                stash_copy(q, slot).start()
    for slot in range(SPLIT):
        @pl.when(slot < count)
        def _():
            for q in range(4):
                stash_copy(q, slot).wait()
    for hop in range(SPLIT):
        @pl.when(hop < count)
        def _():
            for c in order:
                late_copy(c, hop, hop == 0).wait()
                if hop + 1 < SPLIT:
                    pl.when(hop + 1 < count)(lambda: late_copy(c, hop + 1, False).start())
                turn(c, hop)


def scoped_late_kernel(n_rows, depth, chunks, per_ring, *refs):
    sem = pltpu.SemaphoreType.DMA
    pl.run_scoped(
        functools.partial(late_kernel, n_rows, depth, chunks, per_ring, *refs),
        sem((chunks,)), sem((SPLIT, chunks)), sem((SPLIT, 4)),
    )


def write_kernel(pieces, held_ref, norm_ref, out_ref, norm_out_ref, sems):
    rows = held_ref.shape[0] // pieces
    copies = []
    for i in range(pieces):
        part = pl.ds(i * rows, rows)
        copies.append(pltpu.make_async_copy(held_ref.at[part, :], out_ref.at[part, :], sems.at[i]))
        copies[-1].start()
    copies.append(pltpu.make_async_copy(norm_ref, norm_out_ref, sems.at[pieces]))
    copies[-1].start()
    for copy in copies:
        copy.wait()


def patch_kernel(n_rows, depth, quarter, patch_ref, first_ref, out_ref, sems):
    me = lax.axis_index("rows")
    count = splits(lax.axis_index("tp"))

    def each(act):
        for slot in range(SPLIT):
            @pl.when(slot < count)
            def _():
                for q in range(4):
                    origin, gap = late_place(n_rows, q, me, slot + 1)
                    odd = origin % 2
                    base = origin // 2 * 2 * depth
                    rows = pl.ds(q * quarter, quarter)
                    last = (gap <= slot) | (gap > count)

                    def copy(start, to, lanes):
                        return pltpu.make_async_copy(
                            patch_ref.at[slot, rows, pl.ds(start, lanes)],
                            out_ref.at[rows, pl.ds(pl.multiple_of(to, LANES), lanes)],
                            sems.at[slot, q])

                    @pl.when(last)
                    def _():
                        act(copy(0, base + odd * 256, 384))

                    @pl.when(jnp.logical_not(last))
                    def _():
                        act(copy(pl.multiple_of(odd * LANES, LANES), base + odd * 384, 256))

    each(lambda copy: copy.start())
    each(lambda copy: copy.wait())


def per_device(train_up, low_up, high_up, norm_train, norm_step):
    n_rows, n_tp = lax.axis_size("rows"), lax.axis_size("tp")
    depth, width = train_up.shape
    rank, own = low_up.shape[1], norm_train.shape[0]
    chunks = width // LANES
    per_ring = chunks // 4
    norm_shape = (n_rows * n_tp * own // LANES, LANES)
    anywhere, vmem = pl.BlockSpec(memory_space=pl.ANY), pl.BlockSpec(memory_space=pltpu.VMEM)
    held, mine, norm = pl.pallas_call(
        functools.partial(scoped_kernel, n_rows, n_tp, depth, chunks, per_ring),
        out_shape=(
            pltpu.VMEM((width, n_rows * depth), jnp.bfloat16),
            pltpu.VMEM((chunks, depth, LANES), jnp.bfloat16),
            pltpu.VMEM(norm_shape, jnp.bfloat16),
        ),
        in_specs=[anywhere] * 5,
        out_specs=(vmem, vmem, vmem),
        scratch_shapes=[
            pltpu.VMEM((chunks, depth, LANES), jnp.bfloat16),
            pltpu.VMEM((rank, depth), jnp.bfloat16),
            pltpu.VMEM((rank, width), jnp.bfloat16),
            pltpu.VMEM((2, 1, own), jnp.float32),
            pltpu.VMEM((chunks, n_rows * depth, LANES), jnp.bfloat16),
            pltpu.VMEM((n_rows * n_tp, 1, LANES), jnp.float32),
            pltpu.VMEM(norm_shape, jnp.float32),
            pltpu.VMEM(norm_shape, jnp.bfloat16),
        ],
        compiler_params=pltpu.CompilerParams(
            collective_id=0, has_side_effects=True, vmem_limit_bytes=30 * 1024 * 1024
        ),
    )(train_up, low_up.T, high_up, norm_train.reshape(1, -1), norm_step.reshape(1, -1))
    pieces = 16
    first, norm = pl.pallas_call(
        functools.partial(write_kernel, pieces),
        out_shape=(
            jax.ShapeDtypeStruct(held.shape, held.dtype),
            jax.ShapeDtypeStruct(norm_shape, jnp.bfloat16),
        ),
        in_specs=[anywhere, anywhere],
        out_specs=(anywhere, anywhere),
        scratch_shapes=[pltpu.SemaphoreType.DMA((pieces + 1,))],
        compiler_params=pltpu.CompilerParams(vmem_limit_bytes=1024 * 1024),
    )(held, norm)
    patch = pl.pallas_call(
        functools.partial(scoped_late_kernel, n_rows, depth, chunks, per_ring),
        out_shape=pltpu.VMEM((SPLIT, width, 384), jnp.bfloat16),
        in_specs=[anywhere, vmem],
        out_specs=vmem,
        scratch_shapes=[
            pltpu.VMEM((SPLIT, chunks, depth, LANES), jnp.bfloat16),
            pltpu.VMEM((SPLIT, width, LANES), jnp.bfloat16),
        ],
        compiler_params=pltpu.CompilerParams(
            collective_id=1, has_side_effects=True, vmem_limit_bytes=40 * 1024 * 1024
        ),
    )(first, mine)
    ready = pl.pallas_call(
        functools.partial(patch_kernel, n_rows, depth, width // 4),
        out_shape=jax.ShapeDtypeStruct(held.shape, held.dtype),
        in_specs=[anywhere, anywhere],
        out_specs=anywhere,
        input_output_aliases={1: 0},
        scratch_shapes=[pltpu.SemaphoreType.DMA((SPLIT, 4))],
        compiler_params=pltpu.CompilerParams(vmem_limit_bytes=1024 * 1024),
    )(patch, first)
    return ready, norm.reshape(-1)


def solution(mesh):
    placed = (P("rows", "tp"), P("rows", None), P(None, "tp"), P(("rows", "tp")), P(("rows", "tp")))
    return jax.shard_map(
        per_device, mesh=mesh, in_specs=placed, out_specs=(P("tp", None), P()), check_vma=False
    )
```
